128 devices in a mesh: batch: 8 (over z, y_hi), seq: 16 (over x, y_lo, core).
Axes of the slice: x: 4, y: 4 (y_hi: 2, y_lo: 2; y = y_hi * 2 + y_lo), z: 4, core: 2. Of those that a mesh axis runs over, the one named last changes fastest.
Arguments:
- tokens: bfloat16 [40960, 8192], P(('batch', 'seq')), may hold values from -24 to 24
- out_grad: bfloat16 [40960, 8192], P(('batch', 'seq')), may hold values from -0.109375 to 0.109375
- gate_pre: bfloat16 [40960, 768], P(('batch', 'seq')), may hold values from -8 to 8
- up_pre: bfloat16 [40960, 768], P(('batch', 'seq')), may hold values from -6 to 6
- hidden_grad: bfloat16 [40960, 768], P(('batch', 'seq')), may hold values from -0.03125 to 0.03125
Outputs:
- gate_weight_grad: float32 [8192, 768], P(('seq', 'batch'))
- up_weight_grad: float32 [8192, 768], P(('seq', 'batch'))
- down_weight_grad: float32 [8192, 768], P(('seq', 'batch'))
The draws below stay inside these ranges and needn't reach their ends.
All inputs are finite; a program needn't handle non-finite values.
Results may differ from the reference program's by a relative error of at most 0.019.
Values may be sent and summed in bfloat16 or wider, within the bound.
A program may use at most 192 MiB of HBM per device.

```python
import jax
import jax.numpy as jnp
from jax import lax

D = 8192
FF = 768
TOK_DEV = 320
TOKENS = 40960
N_BATCH = 8
N_SEQ = 16


def strengthened(result, stream_key, source, target, blocks, factor):
    owner, partner = [(jnp.arange(result.shape[position]) // (result.shape[position] // blocks)).reshape([-1 if axis == position else 1 for axis in range(result.ndim)]) for position in (source, target)]
    chosen = jax.random.permutation(stream_key, blocks)[partner]
    strong = (owner == chosen) | (owner == (partner + blocks // 2) % blocks)
    return jnp.where(strong, factor * result, result)


def shard_levels(rng, shape, cuts, smallest, top_value):
    factor_of, own = 1.0, jax.random.fold_in(rng, 6)
    for position, blocks in cuts:
        steps = jnp.exp(jax.random.uniform(jax.random.fold_in(own, position), (blocks,), jnp.float32, smallest / len(cuts), top_value / len(cuts)))
        factor_of = factor_of * jnp.repeat(steps, shape[position] // blocks).reshape([-1 if axis == position else 1 for axis in range(len(shape))])
    return factor_of


def gaussian(own_key, extent, deviation, reach, split=(), kind=jnp.bfloat16):
    array = deviation * jax.random.normal(own_key, extent, jnp.float32)
    if split:
        array = array * shard_levels(own_key, extent, split, -0.22, 0.18)
    return jnp.clip(array, -reach, reach).astype(kind)


def heavy_noise(own_key, extent, width, most, split, heavy, kind=jnp.bfloat16):
    entries = width * jax.random.normal(own_key, extent, jnp.float32)
    if split:
        entries = entries * shard_levels(own_key, extent, split, -0.22, 0.18)
    return jnp.clip(strengthened(entries, jax.random.fold_in(own_key, 3), *heavy), -most, most).astype(kind)


def setup_inputs(seed: int = 0) -> dict:
    key_of = jax.random.split(jax.random.key(seed), 6)
    tokens = heavy_noise(key_of[0], (TOKENS, D), 1.0, 24.0, ((0, 128),), (0, 1, 128, 5.5))
    out_grad = heavy_noise(key_of[1], (TOKENS, D), TOKENS ** -0.5, 0.109375, ((0, 128),), (0, 1, 128, 5.5))
    gate_pre = gaussian(key_of[2], (TOKENS, FF), 1.5, 8.0, ((0, 128),))
    up_pre = gaussian(key_of[3], (TOKENS, FF), 1.0, 6.0, ((0, 128),))
    hidden_grad = gaussian(key_of[4], (TOKENS, FF), TOKENS ** -0.5, 0.03125, ((0, 128),))
    return {"tokens": tokens, "out_grad": out_grad, "gate_pre": gate_pre, "up_pre": up_pre, "hidden_grad": hidden_grad}


def hidden_parts(gate_pre, up_pre, hidden_grad):
    gate_val = gate_pre.astype(jnp.float32)
    up_val = up_pre.astype(jnp.float32)
    grad_val = hidden_grad.astype(jnp.float32)
    sigmoid_val = jax.nn.sigmoid(gate_val)
    activated = gate_val * sigmoid_val
    hidden = (activated * up_val).astype(jnp.bfloat16)
    up_cotangent = (grad_val * activated).astype(jnp.bfloat16)
    gate_cotangent = (grad_val * up_val * sigmoid_val * (1.0 + gate_val * (1.0 - sigmoid_val))).astype(jnp.bfloat16)
    return hidden, gate_cotangent, up_cotangent


def contract_rows(left, right):
    return lax.dot_general(left, right, (((0,), (0,)), ((), ())), preferred_element_type=jnp.float32)


def reference(tokens, out_grad, gate_pre, up_pre, hidden_grad):
    hidden, gate_cotangent, up_cotangent = hidden_parts(gate_pre, up_pre, hidden_grad)
    cotangents = jnp.concatenate([gate_cotangent, up_cotangent], axis=1)
    blocks = N_BATCH * N_SEQ
    model_width = tokens.shape[1]
    hidden_width = hidden.shape[1]

    def add_block(total, pieces):
        features, grads, cotangent_rows, hidden_slice = pieces
        term = jnp.concatenate([contract_rows(features, cotangent_rows), contract_rows(grads, hidden_slice)], axis=1)
        return total + lax.optimization_barrier(term.astype(jnp.bfloat16)).astype(jnp.float32), None

    pieces = (tokens.reshape(blocks, TOK_DEV, model_width), out_grad.reshape(blocks, TOK_DEV, model_width),
              cotangents.reshape(blocks, TOK_DEV, 2 * hidden_width), hidden.reshape(blocks, TOK_DEV, hidden_width))
    total, unused = lax.scan(add_block, jnp.zeros((model_width, 3 * hidden_width), jnp.float32), pieces)
    return (total[:, :hidden_width], total[:, hidden_width:2 * hidden_width], total[:, 2 * hidden_width:])
```

```python
import functools

import jax
import jax.numpy as jnp
from jax import lax
from jax.experimental import pallas as pl
from jax.experimental.pallas import tpu as pltpu
from jax.sharding import Mesh
from jax.sharding import PartitionSpec as P

AXES = ("z", "yh", "x", "yl", "c")
ORDERS = ("xyz", "yzx", "zxy")
MESH = pl.DeviceIdType.MESH
F32, BF16 = jnp.float32, jnp.bfloat16

SUBS = 3
def schedule():
    s = []
    for p in range(3):
        s.append(("C", p, 0, 0))
    for p in range(3):
        s.append(("C", p, 1, 0))
    for p in range(3):
        s += [("E1", p, 0, 0), ("M", p, 1, 0)]
    for p in range(3):
        s.append(("C", p, 2, 0))
    for p in range(3):
        s += [("E2", p, 0, 0), ("M", p, 0, 1)]
    for p in range(3):
        s += [("E1", p, 1, 0), ("M", p, 2, 0)]
    for p in range(3):
        s += [("E1", p, 0, 1)]
    for p in range(3):
        s += [("E2", p, 0, 1), ("M", p, 0, 2)]
    for p in range(3):
        s += [("E2", p, 1, 0), ("M", p, 1, 1)]
    for p in range(3):
        s += [("E1", p, 0, 2)]
    for p in range(3):
        s += [("E2", p, 0, 2)]
    for p in range(3):
        s += [("E1", p, 2, 0)]
    for p in range(3):
        s += [("E1", p, 1, 1)]
    for p in range(3):
        s += [("E2", p, 1, 1), ("M", p, 1, 2)]
    for p in range(3):
        s += [("E1", p, 1, 2)]
    for p in range(3):
        s += [("E2", p, 1, 2)]
    for ph in range(3):
        if ph:
            for p in range(3):
                s += [("E1", p, 2, ph)]
        for p in range(3):
            s += [("E2", p, 2, ph)]
            if ph < 2:
                s += [("M", p, 2, ph + 1)]
    return s


def kernel(tokens, out_grad, gate_pre, up_pre, hidden_grad, out0, out1, out2,
           tok, raw, hb, part, r0, r1, r2, send_sem, recv_sem, in_sem, xs_sem, xr_sem):
    outs = (out0, out1, out2)
    recv = (r0, r1, r2)
    z, yh, x, yl, c = (lax.axis_index(a) for a in AXES)
    y = yh * 2 + yl
    me = {"x": x, "y": y, "z": z}
    n_tok = tokens.shape[0]
    cols = hb.shape[3]
    tile = tok.shape[3]
    n_tile = tok.shape[1]
    rows = part.shape[5]
    step = {}
    for d in "xyz":
        step[d] = tuple(lax.rem(me[d] + k, 4) for k in range(4))

    def device(d, k):
        at = dict(me)
        at[d] = step[d][k]
        return (at["z"], lax.div(at["y"], 2), at["x"], lax.rem(at["y"], 2), c)

    partner = (z, yh, x, yl, 1 - c)

    own = []
    raws = (gate_pre, up_pre, hidden_grad)
    for i, ref in enumerate(raws):
        own.append(pltpu.make_async_copy(ref, raw.at[i, pl.ds(0, n_tok)], in_sem.at[i]))
    bigs = (tokens, out_grad)
    for w, ref in enumerate(bigs):
        for m in range(n_tile):
            at = pl.multiple_of((m * 2 + c) * tile, tile)
            own.append(pltpu.make_async_copy(
                ref.at[:, pl.ds(at, tile)], tok.at[w, m, pl.ds(0, n_tok)], in_sem.at[3 + w * n_tile + m]))
    for cp in own:
        cp.start()

    barrier = pltpu.get_barrier_semaphore()
    pl.semaphore_signal(barrier, inc=1, device_id=partner, device_id_type=MESH)
    for d in "xyz":
        for k in (1, 3):
            pl.semaphore_signal(barrier, inc=1, device_id=device(d, k), device_id_type=MESH)
    pl.semaphore_wait(barrier, 7)

    swap = []
    for i, ref in enumerate(raws):
        swap.append(pltpu.make_async_remote_copy(
            ref, raw.at[i, pl.ds(n_tok, n_tok)], xs_sem.at[i], xr_sem.at[i],
            device_id=partner, device_id_type=MESH))
    for w, ref in enumerate(bigs):
        for m in range(n_tile):
            at = pl.multiple_of((m * 2 + 1 - c) * tile, tile)
            swap.append(pltpu.make_async_remote_copy(
                ref.at[:, pl.ds(at, tile)], tok.at[w, m, pl.ds(n_tok, n_tok)],
                xs_sem.at[3 + w * n_tile + m], xr_sem.at[3 + w * n_tile + m],
                device_id=partner, device_id_type=MESH))
    for cp in swap:
        cp.start()

    piece = 32

    def hidden(j):
        def body(i, carry):
            at = pl.ds(pl.multiple_of(i * piece, piece), piece)
            cs = pl.ds(j * cols, cols)
            gate_val = raw[0, at, cs].astype(F32)
            up_val = raw[1, at, cs].astype(F32)
            grad_val = raw[2, at, cs].astype(F32)
            sig = jax.nn.sigmoid(gate_val)
            activated = gate_val * sig
            hb[2, j, at] = (activated * up_val).astype(BF16)
            hb[1, j, at] = (grad_val * activated).astype(BF16)
            hb[0, j, at] = (grad_val * up_val * sig * (1.0 + gate_val * (1.0 - sig))).astype(BF16)
            return carry
        return body

    descs = {}

    def base(p, j, ph):
        o = ORDERS[p]
        ref = part.at[p, j]
        if ph >= 1:
            ref = ref.at[me[o[0]]]
        if ph >= 2:
            ref = ref.at[me[o[1]]]
        return ref

    def half_of(ref, k, h):
        n = ref.shape[1] // 2
        return ref.at[k, pl.ds(h * n, n)]

    def message(p, j, ph, i, src, direction):
        d = ORDERS[p][ph]
        cp = pltpu.make_async_remote_copy(
            src, recv[ph].at[p, j, i], send_sem.at[p, j, ph, i], recv_sem.at[p, j, ph, i],
            device_id=device(d, direction), device_id_type=MESH)
        cp.start()
        descs[(p, j, ph, i)] = cp

    def send_far(p, j, ph):
        b = base(p, j, ph)
        s = step[ORDERS[p][ph]]
        message(p, j, ph, 0, half_of(b, s[2], 0), 1)
        message(p, j, ph, 1, half_of(b, s[2], 1), 3)

    def send_near(p, j, ph):
        b = base(p, j, ph)
        s = step[ORDERS[p][ph]]
        message(p, j, ph, 2, half_of(b, s[1], 1), 1)
        message(p, j, ph, 3, half_of(b, s[3], 0), 3)

    arrived = set()

    def need(key, copies):
        if key not in arrived:
            arrived.add(key)
            for cp in copies:
                cp()

    def matmul(p, j, ms):
        w = 1 if p == 2 else 0
        o = ORDERS[p]

        def one(m):
            res = lax.dot_general(tok[w, m], hb[p, j], (((0,), (0,)), ((), ())),
                                  preferred_element_type=F32).astype(BF16)
            mx = lax.div(m, 2)
            ml = lax.rem(m, 2)
            for zz in range(4):
                for hh in range(2):
                    at = {"x": mx, "y": hh * 2 + ml, "z": zz}
                    lo = (zz * 2 + hh) * rows
                    part[p, j, at[o[0]], at[o[1]], at[o[2]]] = res[lo:lo + rows]

        n, f = ms

        def body(i, carry):
            one(f(i))
            return carry
        lax.fori_loop(0, n, body, 0)

    def compute(p, j, send):
        if p == 0:
            if j == 0:
                for i in range(3):
                    own[i].wait()
                    swap[i].wait_recv()
            lax.fori_loop(0, 2 * n_tok // piece, hidden(j), 0)
        if j == 0 and p in (0, 2):
            w = p // 2
            for m in range(n_tile):
                own[3 + w * n_tile + m].wait()
                swap[3 + w * n_tile + m].wait_recv()
        if p == 0 and send:
            s = step["x"]
            matmul(p, j, (2, lambda i: s[2] * 2 + i))
            send_far(p, j, 0)
            matmul(p, j, (4, lambda i: lax.rem(s[1] + 2 * lax.div(i, 2), 4) * 2 + lax.rem(i, 2)))
            send_near(p, j, 0)
            matmul(p, j, (2, lambda i: s[0] * 2 + i))
        elif p == 1 and send:
            matmul(p, j, (4, lambda i: i * 2 + yl))
            send_far(p, j, 0)
            matmul(p, j, (4, lambda i: i * 2 + 1 - yl))
            send_near(p, j, 0)
        else:
            matmul(p, j, (n_tile, lambda i: i))
            if send:
                send_far(p, j, 0)
                send_near(p, j, 0)

    def relay(p, j, ph):
        b = base(p, j, ph)
        s = step[ORDERS[p][ph]]
        for i, k in ((0, 1), (1, 3)):
            descs[(p, j, ph, i)].wait_recv()
            got = recv[ph].at[p, j, i]
            mine = half_of(b, s[k], i)
            add(got, (mine,), got)
            message(p, j, ph, 4 + i, got, k)

    def add(first, others, dst):
        shape = dst.shape
        lead = shape[:-2]
        count = 1
        for n in lead:
            count *= n

        def block(ix):
            v = first[ix].astype(F32)
            for o in others:
                v = v + o[ix].astype(F32)
            dst[ix] = v.astype(dst.dtype)

        if count == 1 and not lead:
            block((slice(None), slice(None)))
            return

        def body(i, carry):
            if len(lead) == 1:
                block((i,))
            else:
                block((lax.div(i, lead[1]), lax.rem(i, lead[1])))
            return carry
        lax.fori_loop(0, count, body, 0)

    def finish(p, j, ph):
        b = base(p, j, ph)
        s = step[ORDERS[p][ph]]
        for i in (2, 3, 4, 5):
            descs[(p, j, ph, i)].wait_recv()
        got = recv[ph]
        for h, (i, k) in enumerate(((3, 4), (2, 5))):
            mine = half_of(b, s[0], h)
            if ph < 2:
                dst = mine
            else:
                n = rows // 2
                dst = outs[p].at[pl.ds(h * n, n), pl.ds(j * cols, cols)]
            add(mine, (got.at[p, j, i], got.at[p, j, k]), dst)

    for op, p, j, ph in schedule():
        if op == "C":
            compute(p, j, j == 0)
        elif op == "M":
            send_far(p, j, ph)
            send_near(p, j, ph)
        elif op == "E1":
            relay(p, j, ph)
        else:
            finish(p, j, ph)

    for cp in swap:
        cp.wait_send()
    for cp in descs.values():
        cp.wait_send()


def on_device(tokens, out_grad, gate_pre, up_pre, hidden_grad):
    n_tok, width = tokens.shape
    hid = gate_pre.shape[1]
    rows = width // 128
    cols = hid // SUBS
    tile = width // 16
    dma = pltpu.SemaphoreType.DMA
    any_spec = pl.BlockSpec(memory_space=pl.ANY)
    vmem = pl.BlockSpec(memory_space=pltpu.VMEM)
    out = jax.ShapeDtypeStruct((rows, hid), F32)
    n_in = 3 + 16
    return pl.pallas_call(
        kernel,
        out_shape=(out,) * 3,
        in_specs=[any_spec] * 5,
        out_specs=(vmem,) * 3,
        scratch_shapes=[
            pltpu.VMEM((2, 8, 2 * n_tok, tile), BF16),
            pltpu.VMEM((3, 2 * n_tok, hid), BF16),
            pltpu.VMEM((3, SUBS, 2 * n_tok, cols), BF16),
            pltpu.VMEM((3, SUBS, 4, 4, 4, rows, cols), BF16),
            pltpu.VMEM((3, SUBS, 6, 2, 4, rows, cols), BF16),
            pltpu.VMEM((3, SUBS, 6, 2, rows, cols), BF16),
            pltpu.VMEM((3, SUBS, 6, rows // 2, cols), BF16),
            dma((3, SUBS, 3, 6)),
            dma((3, SUBS, 3, 6)),
            dma((n_in,)),
            dma((n_in,)),
            dma((n_in,)),
        ],
        compiler_params=pltpu.CompilerParams(
            collective_id=0, has_side_effects=True, vmem_limit_bytes=67043328),
        name="grad_sum",
    )(tokens, out_grad, gate_pre, up_pre, hidden_grad)


def solution(mesh):
    split = Mesh(mesh.devices.reshape(4, 2, 4, 2, 2), AXES)
    spec_in = P(AXES, None)
    spec_out = P(("x", "yl", "c", "z", "yh"), None)
    return jax.shard_map(
        on_device, mesh=split, in_specs=(spec_in,) * 5, out_specs=(spec_out,) * 3, check_vma=False
    )
```

```python
import jax
import jax.numpy as jnp
from jax import lax
from jax.experimental import pallas as pl
from jax.experimental.pallas import tpu as pltpu
from jax.sharding import Mesh
from jax.sharding import PartitionSpec as P

AXES = ("z", "yh", "x", "yl", "c")
DIM_ORDERS = ("xyz", "yzx", "zxy")
MESH = pl.DeviceIdType.MESH
F32, BF16 = jnp.float32, jnp.bfloat16

BLOCKS = (
    (0, 0, 0, (256,)),
    (1, 0, 1, (256,)),
    (0, 256, 2, (256,)),
    (1, 256, 0, (256,)),
    (0, 512, 1, (256,)),
    (1, 512, 2, (256,)),
    (2, 0, 0, (256,)),
    (2, 256, 1, (256,)),
    (2, 512, 2, (256,)),
)
ORDER = (
    (0, 0, 0), (0, 1, 0), (0, 2, 0), (0, 0, 1), (0, 1, 1), (1, 0, 0), (0, 0, 2), (0, 3, 0),
    (1, 1, 0), (0, 3, 1), (0, 3, 2), (0, 4, 0), (0, 4, 1), (1, 2, 0), (0, 5, 0), (0, 6, 0),
    (0, 6, 1), (0, 6, 2), (0, 7, 0), (0, 7, 1), (0, 8, 0), (2, 0, 0), (2, 1, 0), (1, 3, 0),
    (2, 2, 0), (1, 4, 0), (1, 5, 0), (1, 6, 0), (1, 7, 0), (1, 8, 0), (1, 0, 1), (2, 3, 0),
    (1, 1, 1), (1, 2, 1), (2, 4, 0), (2, 5, 0), (2, 6, 0), (2, 7, 0), (2, 2, 1), (2, 0, 1),
    (1, 5, 1), (1, 3, 1), (2, 8, 0), (2, 1, 1), (1, 6, 1), (1, 4, 1), (2, 5, 1), (1, 2, 2),
    (1, 8, 1), (1, 7, 1), (2, 3, 1), (1, 1, 2), (1, 0, 2), (2, 6, 1), (1, 5, 2), (2, 2, 2),
    (2, 4, 1), (2, 8, 1), (2, 7, 1), (2, 1, 2), (1, 3, 2), (2, 5, 2), (2, 0, 2), (1, 6, 2),
    (1, 4, 2), (1, 8, 2), (1, 7, 2), (2, 3, 2), (2, 6, 2), (2, 4, 2), (2, 8, 2), (2, 7, 2),
)
CHUNKS = tuple(
    (b[0], b[1] + sum(b[3][:i]), w, DIM_ORDERS[b[2]]) for b in BLOCKS for i, w in enumerate(b[3]))
BLOCK_CHUNKS = tuple(
    tuple(sum(len(a[3]) for a in BLOCKS[:n]) + i for i in range(len(b[3]))) for n, b in enumerate(BLOCKS))
RAW = 256
PIECE = 32


def kernel(*refs):
    tokens, out_grad, gate_pre, up_pre, hidden_grad = refs[:5]
    outs = refs[5:8]
    tok, raw, hb = refs[8:11]
    n_chunk = len(CHUNKS)
    part = refs[11:11 + n_chunk]
    recv = tuple(refs[11 + (1 + ph) * n_chunk:11 + (2 + ph) * n_chunk] for ph in range(3))
    send_sem, recv_sem, in_sem, xs_sem, xr_sem = refs[11 + 4 * n_chunk:]

    z, yh, x, yl, c = (lax.axis_index(a) for a in AXES)
    y = yh * 2 + yl
    me = {"x": x, "y": y, "z": z}
    n_tok = tokens.shape[0]
    n_slot, tile = tok.shape[1], tok.shape[3]
    n_raw = raw.shape[0]
    rows = part[0].shape[3]
    step = {d: tuple(lax.rem(me[d] + k, 4) for k in range(4)) for d in "xyz"}

    def device(d, k):
        at = dict(me)
        at[d] = step[d][k]
        return (at["z"], lax.div(at["y"], 2), at["x"], lax.rem(at["y"], 2), c)

    partner = (z, yh, x, yl, 1 - c)

    def slot_at(slot):
        return lax.rem(x + 2 + lax.div(slot, 2), 4), lax.rem(yl + lax.rem(slot, 2), 2)

    raws = (gate_pre, up_pre, hidden_grad)
    bigs = (tokens, out_grad)

    def pieces(core):
        found = {}
        for j in range(n_raw):
            for i, ref in enumerate(raws):
                found[("raw", j, i)] = (ref.at[:, pl.ds(j * RAW, RAW)], lambda r, j=j, i=i: raw.at[j, i, r])
        for w, ref in enumerate(bigs):
            for s in range(n_slot):
                sx, sl = slot_at(s)
                at = pl.multiple_of((sx * 4 + sl * 2 + core) * tile, tile)
                found[("big", w, s)] = (ref.at[:, pl.ds(at, tile)], lambda r, w=w, s=s: tok.at[w, s, r])
        return found

    names = [("raw", 0, i) for i in range(3)] + [("big", 0, s) for s in range(n_slot)]
    names += [("raw", j, i) for j in range(1, n_raw) for i in range(3)] + [("big", 1, s) for s in range(n_slot)]
    mine, theirs = pieces(c), pieces(1 - c)
    own, swap = {}, {}
    for n, name in enumerate(names):
        src, dst = mine[name]
        own[name] = pltpu.make_async_copy(src, dst(pl.ds(0, n_tok)), in_sem.at[n])
        own[name].start()

    barrier = pltpu.get_barrier_semaphore()
    pl.semaphore_signal(barrier, inc=1, device_id=partner, device_id_type=MESH)
    for d in "xyz":
        for k in (1, 3):
            pl.semaphore_signal(barrier, inc=1, device_id=device(d, k), device_id_type=MESH)
    pl.semaphore_wait(barrier, 7)

    for n, name in enumerate(names):
        src, dst = theirs[name]
        swap[name] = pltpu.make_async_remote_copy(
            src, dst(pl.ds(n_tok, n_tok)), xs_sem.at[n], xr_sem.at[n], device_id=partner, device_id_type=MESH)
        swap[name].start()

    have = set()

    def need(name):
        if name not in have:
            have.add(name)
            own[name].wait()
            swap[name].wait_recv()

    def hidden(j):
        if ("hidden", j) in have:
            return
        have.add(("hidden", j))
        for i in range(3):
            need(("raw", j, i))

        def body(i, carry):
            at = pl.ds(pl.multiple_of(i * PIECE, PIECE), PIECE)
            cs = pl.ds(j * RAW, RAW)
            gate_val = raw[j, 0, at].astype(F32)
            up_val = raw[j, 1, at].astype(F32)
            grad_val = raw[j, 2, at].astype(F32)
            sig = jax.nn.sigmoid(gate_val)
            activated = gate_val * sig
            hb[2, at, cs] = (activated * up_val).astype(BF16)
            hb[1, at, cs] = (grad_val * activated).astype(BF16)
            hb[0, at, cs] = (grad_val * up_val * sig * (1.0 + gate_val * (1.0 - sig))).astype(BF16)
            return carry

        lax.fori_loop(0, 2 * n_tok // PIECE, body, 0)

    copies = {}

    def base(k, ph):
        ref = part[k]
        for d in CHUNKS[k][3][:ph]:
            ref = ref.at[me[d]]
        return ref

    def half_of(ref, i, h):
        n = ref.shape[1] // 2
        return ref.at[i, pl.ds(h * n, n)]

    def send(k, ph, i, src, direction):
        copies[(k, ph, i)] = pltpu.make_async_remote_copy(
            src, recv[ph][k].at[i], send_sem.at[k, ph, i], recv_sem.at[k, ph, i],
            device_id=device(CHUNKS[k][3][ph], direction), device_id_type=MESH)
        copies[(k, ph, i)].start()

    def send_far(k, ph):
        s = step[CHUNKS[k][3][ph]]
        send(k, ph, 0, half_of(base(k, ph), s[2], 0), 1)
        send(k, ph, 1, half_of(base(k, ph), s[2], 1), 3)

    def send_near(k, ph):
        s = step[CHUNKS[k][3][ph]]
        send(k, ph, 2, half_of(base(k, ph), s[1], 1), 1)
        send(k, ph, 3, half_of(base(k, ph), s[3], 0), 3)

    near = lambda i: 2 + 4 * lax.div(i, 2) + lax.rem(i, 2)
    parts_of = (
        ((2, lambda i: i), (4, near), (2, lambda i: 4 + i)),
        ((4, lambda i: 2 * i), (4, lambda i: 2 * i + 1)),
        ((n_slot, lambda i: i),),
    )
    slots_of = (
        ((0, 1), (2, 3, 6, 7), (4, 5)), ((0, 2, 4, 6), (1, 3, 5, 7)), (tuple(range(8)),))

    def multiply(b, seg):
        p, first, dim, widths = BLOCKS[b]
        w = p // 2
        for j in range(first // RAW, (first + sum(widths) - 1) // RAW + 1):
            hidden(j)
        for s in slots_of[dim][seg]:
            need(("big", w, s))
        count, slot_of = parts_of[dim][seg]

        def body(i, carry):
            slot = slot_of(i)
            res = lax.dot_general(
                tok[w, slot], hb[p, :, pl.ds(first, sum(widths))], (((0,), (0,)), ((), ())),
                preferred_element_type=F32).astype(BF16)
            sx, sl = slot_at(slot)
            for k in BLOCK_CHUNKS[b]:
                lane = CHUNKS[k][1] - first
                for sz in range(4):
                    for sh in range(2):
                        at = {"x": sx, "y": sh * 2 + sl, "z": sz}
                        lo = (sz * 2 + sh) * rows
                        o = CHUNKS[k][3]
                        part[k][at[o[0]], at[o[1]], at[o[2]]] = res[lo:lo + rows, lane:lane + CHUNKS[k][2]]
            return carry

        lax.fori_loop(0, count, body, 0)
        for k in BLOCK_CHUNKS[b]:
            if seg == 0:
                send_far(k, 0)
            if seg == 1 or len(parts_of[dim]) == 1:
                send_near(k, 0)

    def add(first, others, dst):
        lead = dst.shape[:-2]
        count = 1
        for n in lead:
            count *= n

        def block(ix):
            v = first[ix].astype(F32)
            for o in others:
                v = v + o[ix].astype(F32)
            dst[ix] = v.astype(dst.dtype)

        if not lead:
            block((slice(None), slice(None)))
            return

        def body(i, carry):
            block((i,) if len(lead) == 1 else (lax.div(i, lead[1]), lax.rem(i, lead[1])))
            return carry

        lax.fori_loop(0, count, body, 0)

    def relay(k, ph):
        s = step[CHUNKS[k][3][ph]]
        for i, to in ((0, 1), (1, 3)):
            copies[(k, ph, i)].wait_recv()
            got = recv[ph][k].at[i]
            add(got, (half_of(base(k, ph), s[to], i),), got)
            send(k, ph, 4 + i, got, to)

    def finish(k, ph):
        p, first, width, o = CHUNKS[k]
        got = recv[ph][k]
        for h, pair in enumerate(((3, 4), (2, 5))):
            for i in pair:
                copies[(k, ph, i)].wait_recv()
            own_half = half_of(base(k, ph), me[o[ph]], h)
            if ph < 2:
                dst = own_half
            else:
                dst = outs[p].at[pl.ds(h * (rows // 2), rows // 2), pl.ds(first, width)]
            add(own_half, tuple(got.at[i] for i in pair), dst)
        if ph < 2:
            send_far(k, ph + 1)
            send_near(k, ph + 1)

    for op, n, m in ORDER:
        (multiply, relay, finish)[op](n, m)

    for cp in swap.values():
        cp.wait_send()
    for cp in copies.values():
        cp.wait_send()


def on_device(tokens, out_grad, gate_pre, up_pre, hidden_grad):
    n_tok, width = tokens.shape
    hid = gate_pre.shape[1]
    rows = width // 128
    tile = width // 16
    dma = pltpu.SemaphoreType.DMA
    any_spec = pl.BlockSpec(memory_space=pl.ANY)
    vmem = pl.BlockSpec(memory_space=pltpu.VMEM)
    out = jax.ShapeDtypeStruct((rows, hid), F32)
    widths = [k[2] for k in CHUNKS]
    n_in = 3 * (hid // RAW) + 16
    return pl.pallas_call(
        kernel,
        out_shape=(out,) * 3,
        in_specs=[any_spec] * 5,
        out_specs=(vmem,) * 3,
        scratch_shapes=[
            pltpu.VMEM((2, 8, 2 * n_tok, tile), BF16),
            pltpu.VMEM((hid // RAW, 3, 2 * n_tok, RAW), BF16),
            pltpu.VMEM((3, 2 * n_tok, hid), BF16),
            *[pltpu.VMEM((4, 4, 4, rows, w), BF16) for w in widths],
            *[pltpu.VMEM((6, 2, 4, rows, w), BF16) for w in widths],
            *[pltpu.VMEM((6, 2, rows, w), BF16) for w in widths],
            *[pltpu.VMEM((6, rows // 2, w), BF16) for w in widths],
            dma((len(CHUNKS), 3, 6)),
            dma((len(CHUNKS), 3, 6)),
            dma((n_in,)),
            dma((n_in,)),
            dma((n_in,)),
        ],
        compiler_params=pltpu.CompilerParams(
            collective_id=0, has_side_effects=True, vmem_limit_bytes=67043328),
        name="grad_sum",
    )(tokens, out_grad, gate_pre, up_pre, hidden_grad)


def solution(mesh):
    split = Mesh(mesh.devices.reshape(4, 2, 4, 2, 2), AXES)
    spec_in = P(AXES, None)
    spec_out = P(("x", "yl", "c", "z", "yh"), None)
    return jax.shard_map(
        on_device, mesh=split, in_specs=(spec_in,) * 5, out_specs=(spec_out,) * 3, check_vma=False
    )
```

```python
import jax
import jax.numpy as jnp
from jax import lax
from jax.experimental import pallas as pl
from jax.experimental.pallas import tpu as pltpu
from jax.sharding import Mesh
from jax.sharding import PartitionSpec as P

AXES = ("z", "yh", "x", "yl", "c")
DIM_ORDERS = ("xyz", "yzx", "zxy", "xzy", "yxz", "zyx")
MESH = pl.DeviceIdType.MESH
F32, BF16 = jnp.float32, jnp.bfloat16

BLOCKS = (
    (0, 0, 0, (256,)),
    (1, 0, 1, (256,)),
    (0, 256, 2, (256,)),
    (1, 256, 0, (256,)),
    (0, 512, 1, (256,)),
    (1, 512, 2, (256,)),
    (2, 0, 0, (256,)),
    (2, 256, 1, (256,)),
    (2, 512, 2, (256,)),
)
ORDER = (
    (0, 3, 0), (3, 3, 0, 0), (0, 1, 0), (3, 1, 0, 0), (0, 2, 0), (3, 2, 0, 0), (0, 1, 1), (0, 6, 0),
    (3, 1, 0, 1), (3, 2, 0, 1), (3, 6, 0, 0), (0, 4, 0), (0, 7, 0), (0, 3, 1), (1, 3, 0), (3, 4, 0, 0),
    (1, 2, 0), (1, 1, 0), (0, 0, 0), (0, 8, 0), (3, 0, 0, 0), (3, 8, 0, 0), (0, 5, 0), (0, 4, 1),
    (3, 3, 0, 1), (0, 6, 1), (3, 7, 0, 0), (3, 5, 0, 0), (0, 0, 1), (3, 6, 0, 1), (1, 6, 0), (3, 8, 0, 1),
    (3, 5, 0, 1), (0, 7, 1), (1, 4, 0), (3, 7, 0, 1), (1, 0, 0), (1, 5, 0), (2, 1, 0), (3, 4, 0, 1),
    (2, 2, 0), (1, 8, 0), (0, 3, 2), (3, 2, 1, 0), (3, 0, 0, 1), (3, 2, 1, 1), (1, 7, 0), (0, 0, 2),
    (3, 1, 1, 0), (0, 6, 2), (2, 4, 0), (2, 3, 0), (2, 6, 0), (3, 6, 1, 0), (3, 3, 1, 1), (2, 5, 0),
    (3, 1, 1, 1), (3, 3, 1, 0), (2, 7, 0), (3, 6, 1, 1), (3, 5, 1, 0), (1, 2, 1), (1, 6, 1), (2, 0, 0),
    (3, 7, 1, 0), (2, 8, 0), (3, 4, 1, 0), (3, 0, 1, 0), (3, 8, 1, 0), (3, 7, 1, 1), (1, 1, 1), (3, 8, 1, 1),
    (2, 2, 1), (3, 5, 1, 1), (3, 4, 1, 1), (1, 5, 1), (1, 3, 1), (3, 0, 1, 1), (1, 4, 1), (1, 0, 1),
    (1, 7, 1), (3, 2, 2, 0), (1, 8, 1), (2, 6, 1), (2, 3, 1), (3, 3, 2, 0), (2, 5, 1), (3, 5, 2, 0),
    (2, 1, 1), (3, 1, 2, 0), (3, 2, 2, 1), (2, 8, 1), (3, 8, 2, 0), (2, 0, 1), (3, 0, 2, 0), (2, 4, 1),
    (3, 4, 2, 0), (1, 2, 2), (3, 6, 2, 0), (3, 1, 2, 1), (2, 7, 1), (3, 7, 2, 0), (3, 5, 2, 1), (1, 5, 2),
    (3, 0, 2, 1), (3, 8, 2, 1), (3, 3, 2, 1), (1, 1, 2), (1, 3, 2), (3, 7, 2, 1), (3, 6, 2, 1), (3, 4, 2, 1),
    (1, 8, 2), (1, 0, 2), (1, 4, 2), (2, 2, 2), (1, 6, 2), (1, 7, 2), (2, 5, 2), (2, 1, 2),
    (2, 3, 2), (2, 8, 2), (2, 0, 2), (2, 6, 2), (2, 4, 2), (2, 7, 2),
)
CHUNKS = tuple(
    (b[0], b[1] + sum(b[3][:i]), w, DIM_ORDERS[b[2]]) for b in BLOCKS for i, w in enumerate(b[3]))
BLOCK_CHUNKS = tuple(
    tuple(sum(len(a[3]) for a in BLOCKS[:n]) + i for i in range(len(b[3]))) for n, b in enumerate(BLOCKS))
RAW = 256
PIECE = 64


def kernel(*refs):
    tokens, out_grad, gate_pre, up_pre, hidden_grad = refs[:5]
    outs = refs[5:8]
    tok, raw, hb = refs[8:11]
    n_chunk = len(CHUNKS)
    part = refs[11:11 + n_chunk]
    recv = tuple(refs[11 + (1 + ph) * n_chunk:11 + (2 + ph) * n_chunk] for ph in range(3))
    send_sem, recv_sem, in_sem, xs_sem, xr_sem = refs[11 + 4 * n_chunk:]

    z, yh, x, yl, c = (lax.axis_index(a) for a in AXES)
    y = yh * 2 + yl
    me = {"x": x, "y": y, "z": z}
    n_tok = tokens.shape[0]
    n_slot, tile = tok.shape[1], tok.shape[3]
    n_raw = raw.shape[0]
    rows = part[0].shape[3]
    step = {d: tuple(lax.rem(me[d] + k, 4) for k in range(4)) for d in "xyz"}

    def device(d, k):
        at = dict(me)
        at[d] = step[d][k]
        return (at["z"], lax.div(at["y"], 2), at["x"], lax.rem(at["y"], 2), c)

    partner = (z, yh, x, yl, 1 - c)

    def slot_at(slot):
        return lax.rem(x + 2 + lax.div(slot, 2), 4), lax.rem(yl + lax.rem(slot, 2), 2)

    raws = (gate_pre, up_pre, hidden_grad)
    bigs = (tokens, out_grad)

    def pieces(core):
        found = {}
        for j in range(n_raw):
            for i, ref in enumerate(raws):
                found[("raw", j, i)] = (ref.at[:, pl.ds(j * RAW, RAW)], lambda r, j=j, i=i: raw.at[j, i, r])
        for w, ref in enumerate(bigs):
            for s in range(n_slot):
                sx, sl = slot_at(s)
                at = pl.multiple_of((sx * 4 + sl * 2 + core) * tile, tile)
                found[("big", w, s)] = (ref.at[:, pl.ds(at, tile)], lambda r, w=w, s=s: tok.at[w, s, r])
        return found

    names = [("raw", j, i) for j in range(2) for i in range(3)] + [("big", 0, s) for s in range(n_slot)]
    names += [("raw", j, i) for j in range(2, n_raw) for i in range(3)] + [("big", 1, s) for s in range(n_slot)]
    mine, theirs = pieces(c), pieces(1 - c)
    own, swap = {}, {}
    for n, name in enumerate(names):
        src, dst = mine[name]
        own[name] = pltpu.make_async_copy(src, dst(pl.ds(0, n_tok)), in_sem.at[n])
        own[name].start()

    barrier = pltpu.get_barrier_semaphore()
    pl.semaphore_signal(barrier, inc=1, device_id=partner, device_id_type=MESH)
    for d in "xyz":
        for k in (1, 3):
            pl.semaphore_signal(barrier, inc=1, device_id=device(d, k), device_id_type=MESH)
    pl.semaphore_wait(barrier, 7)

    for n, name in enumerate(names):
        src, dst = theirs[name]
        swap[name] = pltpu.make_async_remote_copy(
            src, dst(pl.ds(n_tok, n_tok)), xs_sem.at[n], xr_sem.at[n], device_id=partner, device_id_type=MESH)
        swap[name].start()

    have = set()

    def need(name):
        if name not in have:
            have.add(name)
            own[name].wait()
            swap[name].wait_recv()

    def hidden(j):
        if ("hidden", j) in have:
            return
        have.add(("hidden", j))
        for i in range(3):
            need(("raw", j, i))

        def body(i, carry):
            at = pl.ds(pl.multiple_of(i * PIECE, PIECE), PIECE)
            cs = pl.ds(j * RAW, RAW)
            gate_val = raw[j, 0, at].astype(F32)
            up_val = raw[j, 1, at].astype(F32)
            grad_val = raw[j, 2, at].astype(F32)
            sig = jax.nn.sigmoid(gate_val)
            activated = gate_val * sig
            hb[2, at, cs] = (activated * up_val).astype(BF16)
            hb[1, at, cs] = (grad_val * activated).astype(BF16)
            hb[0, at, cs] = (grad_val * up_val * sig * (1.0 + gate_val * (1.0 - sig))).astype(BF16)
            return carry

        lax.fori_loop(0, 2 * n_tok // PIECE, body, 0)

    copies = {}

    def base(k, ph):
        ref = part[k]
        for d in CHUNKS[k][3][:ph]:
            ref = ref.at[me[d]]
        return ref

    def half_of(ref, i, h):
        n = ref.shape[1] // 2
        return ref.at[i, pl.ds(h * n, n)]

    def send(k, ph, i, src, direction):
        copies[(k, ph, i)] = pltpu.make_async_remote_copy(
            src, recv[ph][k].at[i], send_sem.at[k, ph, i], recv_sem.at[k, ph, i],
            device_id=device(CHUNKS[k][3][ph], direction), device_id_type=MESH)
        copies[(k, ph, i)].start()

    def send_far(k, ph):
        s = step[CHUNKS[k][3][ph]]
        send(k, ph, 0, half_of(base(k, ph), s[2], 0), 1)
        send(k, ph, 1, half_of(base(k, ph), s[2], 1), 3)

    def send_near(k, ph):
        s = step[CHUNKS[k][3][ph]]
        send(k, ph, 2, half_of(base(k, ph), s[1], 1), 1)
        send(k, ph, 3, half_of(base(k, ph), s[3], 0), 3)

    parts_of = (
        ((1, lambda i: (0, 1)), (2, lambda i: (2 + 4 * i, 3 + 4 * i)), (1, lambda i: (4, 5))),
        ((2, lambda i: (4 * i, 4 * i + 2)), (2, lambda i: (4 * i + 1, 4 * i + 3))),
        ((4, lambda i: (2 * i, 2 * i + 1)),),
    )
    slots_of = (
        ((0, 1), (2, 3, 6, 7), (4, 5)), ((0, 2, 4, 6), (1, 3, 5, 7)), (tuple(range(8)),))

    def multiply(b, seg):
        p, first, dim, widths = BLOCKS[b]
        dim %= 3
        w = p // 2
        for j in range(first // RAW, (first + sum(widths) - 1) // RAW + 1):
            hidden(j)
        for s in slots_of[dim][seg]:
            need(("big", w, s))
        count, slot_of = parts_of[dim][seg]

        def body(i, carry):
            pair = slot_of(i)
            left = jnp.concatenate([tok[w, s] for s in pair], axis=1)
            res = lax.dot_general(
                left, hb[p, :, pl.ds(first, sum(widths))], (((0,), (0,)), ((), ())),
                preferred_element_type=F32).astype(BF16)
            for t, slot in enumerate(pair):
                sx, sl = slot_at(slot)
                for k in BLOCK_CHUNKS[b]:
                    lane = CHUNKS[k][1] - first
                    for sz in range(4):
                        for sh in range(2):
                            at = {"x": sx, "y": sh * 2 + sl, "z": sz}
                            lo = t * tile + (sz * 2 + sh) * rows
                            o = CHUNKS[k][3]
                            part[k][at[o[0]], at[o[1]], at[o[2]]] = res[lo:lo + rows, lane:lane + CHUNKS[k][2]]
            return carry

        lax.fori_loop(0, count, body, 0)

    def add(first, others, dst):
        lead = dst.shape[:-2]
        count = 1
        for n in lead:
            count *= n

        def block(ix):
            v = first[ix].astype(F32)
            for o in others:
                v = v + o[ix].astype(F32)
            dst[ix] = v.astype(dst.dtype)

        if not lead:
            block((slice(None), slice(None)))
            return

        def body(i, carry):
            block((i,) if len(lead) == 1 else (lax.div(i, lead[1]), lax.rem(i, lead[1])))
            return carry

        lax.fori_loop(0, count, body, 0)

    sent = set()

    def sent_by(k, ph, which):
        for i in which:
            if ph >= 0 and (k, ph, i) not in sent:
                sent.add((k, ph, i))
                copies[(k, ph, i)].wait_send()

    def relay(k, ph):
        sent_by(k, ph - 1, (4, 5))
        s = step[CHUNKS[k][3][ph]]
        for i, to in ((0, 1), (1, 3)):
            copies[(k, ph, i)].wait_recv()
            got = recv[ph][k].at[i]
            add(got, (half_of(base(k, ph), s[to], i),), got)
            send(k, ph, 4 + i, got, to)

    def launch(k, ph, near_side):
        (send_near if near_side else send_far)(k, ph)

    def finish(k, ph):
        sent_by(k, ph, (0, 1, 2, 3))
        p, first, width, o = CHUNKS[k]
        got = recv[ph][k]
        for h, pair in enumerate(((3, 4), (2, 5))):
            for i in pair:
                copies[(k, ph, i)].wait_recv()
            own_half = half_of(base(k, ph), me[o[ph]], h)
            if ph < 2:
                dst = own_half
            else:
                dst = outs[p].at[pl.ds(h * (rows // 2), rows // 2), pl.ds(first, width)]
            add(own_half, tuple(got.at[i] for i in pair), dst)

    for op, n, m, *h in ORDER:
        (multiply, relay, finish, launch)[op](n, m, *h)

    for cp in swap.values():
        cp.wait_send()
    for key, cp in copies.items():
        if key not in sent:
            cp.wait_send()


def hand_out(*refs):
    for src, dst in zip(refs[:3], refs[3:]):
        dst[...] = src[...]


def on_device(tokens, out_grad, gate_pre, up_pre, hidden_grad):
    n_tok, width = tokens.shape
    hid = gate_pre.shape[1]
    rows = width // 128
    tile = width // 16
    dma = pltpu.SemaphoreType.DMA
    any_spec = pl.BlockSpec(memory_space=pl.ANY)
    vmem = pl.BlockSpec(memory_space=pltpu.VMEM)
    out = jax.ShapeDtypeStruct((rows, hid), F32)
    widths = [k[2] for k in CHUNKS]
    n_in = 3 * (hid // RAW) + 16
    sums = pl.pallas_call(
        kernel,
        out_shape=(out,) * 3,
        in_specs=[any_spec] * 5,
        out_specs=(vmem,) * 3,
        scratch_shapes=[
            pltpu.VMEM((2, 8, 2 * n_tok, tile), BF16),
            pltpu.VMEM((hid // RAW, 3, 2 * n_tok, RAW), BF16),
            pltpu.VMEM((3, 2 * n_tok, hid), BF16),
            *[pltpu.VMEM((4, 4, 4, rows, w), BF16) for w in widths],
            *[pltpu.VMEM((6, 2, 4, rows, w), BF16) for w in widths],
            *[pltpu.VMEM((6, 2, rows, w), BF16) for w in widths],
            *[pltpu.VMEM((6, rows // 2, w), BF16) for w in widths],
            dma((len(CHUNKS), 3, 6)),
            dma((len(CHUNKS), 3, 6)),
            dma((n_in,)),
            dma((n_in,)),
            dma((n_in,)),
        ],
        compiler_params=pltpu.CompilerParams(
            collective_id=0, has_side_effects=True, vmem_limit_bytes=67043328),
        name="grad_sum",
    )(tokens, out_grad, gate_pre, up_pre, hidden_grad)
    return pl.pallas_call(
        hand_out, out_shape=(out,) * 3, in_specs=[vmem] * 3, out_specs=(vmem,) * 3, name="hand_out")(*sums)


def solution(mesh):
    split = Mesh(mesh.devices.reshape(4, 2, 4, 2, 2), AXES)
    spec_in = P(AXES, None)
    spec_out = P(("x", "yl", "c", "z", "yh"), None)
    return jax.shard_map(
        on_device, mesh=split, in_specs=(spec_in,) * 5, out_specs=(spec_out,) * 3, check_vma=False
    )
```

```python
import jax
import jax.numpy as jnp
from jax import lax
from jax.experimental import pallas as pl
from jax.experimental.pallas import tpu as pltpu
from jax.sharding import Mesh
from jax.sharding import PartitionSpec as P

AXES = ("z", "yh", "x", "yl", "c")
DIM_ORDERS = ("xyz", "yzx", "zxy", "xzy", "yxz", "zyx")
MESH = pl.DeviceIdType.MESH
F32, BF16 = jnp.float32, jnp.bfloat16

BLOCKS = (
    (0, 0, 2, (256,)),
    (1, 0, 0, (256,)),
    (0, 256, 1, (256,)),
    (1, 256, 2, (256,)),
    (0, 512, 0, (256,)),
    (1, 512, 1, (256,)),
    (2, 0, 2, (256,)),
    (2, 256, 0, (256,)),
    (2, 512, 1, (256,)),
)
ORDER = (
    (0, 0, 0), (3, 0, 0, 0), (0, 1, 0), (3, 1, 0, 0), (0, 2, 0), (3, 2, 0, 0), (0, 0, 1), (0, 3, 0),
    (0, 7, 0), (3, 3, 0, 0), (3, 7, 0, 0), (0, 1, 1), (3, 0, 0, 1), (0, 2, 1), (3, 2, 0, 1), (1, 0, 0),
    (0, 8, 0), (3, 8, 0, 0), (1, 1, 0), (3, 1, 0, 1), (0, 6, 0), (0, 7, 1), (0, 3, 1), (0, 1, 2),
    (0, 4, 0), (0, 4, 1), (3, 3, 0, 1), (1, 2, 0), (3, 6, 0, 0), (3, 4, 0, 0), (0, 6, 1), (0, 5, 0),
    (0, 7, 2), (0, 3, 2), (0, 0, 2), (3, 6, 0, 1), (3, 5, 0, 0), (1, 3, 0), (1, 7, 0), (3, 4, 0, 1),
    (2, 0, 0), (2, 1, 0), (3, 0, 1, 0), (0, 5, 1), (3, 1, 1, 0), (3, 5, 0, 1), (1, 4, 0), (0, 8, 1),
    (1, 5, 0), (1, 8, 0), (1, 6, 0), (3, 8, 0, 1), (2, 2, 0), (0, 4, 2), (3, 2, 1, 0), (3, 7, 0, 1),
    (3, 2, 1, 1), (2, 3, 0), (2, 5, 0), (2, 4, 0), (3, 3, 1, 0), (3, 4, 1, 0), (1, 1, 1), (0, 6, 2),
    (2, 6, 0), (3, 6, 1, 0), (3, 5, 1, 0), (1, 2, 1), (1, 0, 1), (3, 5, 1, 1), (3, 3, 1, 1), (3, 6, 1, 1),
    (2, 7, 0), (3, 4, 1, 1), (1, 3, 1), (2, 8, 0), (3, 8, 1, 0), (3, 8, 1, 1), (1, 6, 1), (3, 7, 1, 0),
    (1, 4, 1), (1, 5, 1), (2, 2, 1), (3, 1, 1, 1), (3, 0, 1, 1), (1, 8, 1), (3, 2, 2, 0), (3, 2, 2, 1),
    (3, 7, 1, 1), (1, 7, 1), (2, 5, 1), (2, 4, 1), (3, 5, 2, 0), (2, 6, 1), (3, 6, 2, 0), (3, 4, 2, 0),
    (2, 3, 1), (2, 1, 1), (3, 6, 2, 1), (3, 1, 2, 0), (3, 3, 2, 0), (2, 0, 1), (1, 2, 2), (2, 8, 1),
    (3, 0, 2, 0), (3, 8, 2, 0), (3, 4, 2, 1), (2, 7, 1), (3, 7, 2, 0), (3, 3, 2, 1), (1, 5, 2), (1, 6, 2),
    (1, 4, 2), (3, 5, 2, 1), (1, 3, 2), (3, 1, 2, 1), (3, 7, 2, 1), (3, 8, 2, 1), (2, 2, 2), (3, 0, 2, 1),
    (1, 8, 2), (1, 1, 2), (1, 0, 2), (1, 7, 2), (2, 6, 2), (2, 4, 2), (2, 3, 2), (2, 8, 2),
    (2, 5, 2), (2, 1, 2), (2, 0, 2), (2, 7, 2),
)
DIRECT = ()
CHUNKS = tuple(
    (b[0], b[1] + sum(b[3][:i]), w, DIM_ORDERS[b[2]]) for b in BLOCKS for i, w in enumerate(b[3]))
BLOCK_CHUNKS = tuple(
    tuple(sum(len(a[3]) for a in BLOCKS[:n]) + i for i in range(len(b[3]))) for n, b in enumerate(BLOCKS))
RAW = 256
PIECE = 64


def kernel(*refs):
    tokens, out_grad, gate_pre, up_pre, hidden_grad = refs[:5]
    outs = refs[5:8]
    tok, raw, hb = refs[8:11]
    n_chunk = len(CHUNKS)
    part = refs[11:11 + n_chunk]
    recv = tuple(refs[11 + (1 + ph) * n_chunk:11 + (2 + ph) * n_chunk] for ph in range(3))
    send_sem, recv_sem, in_sem, xs_sem, xr_sem, out_sem, result = refs[11 + 4 * n_chunk:]

    z, yh, x, yl, c = (lax.axis_index(a) for a in AXES)
    y = yh * 2 + yl
    me = {"x": x, "y": y, "z": z}
    n_tok = tokens.shape[0]
    n_slot, tile = tok.shape[1], tok.shape[3]
    n_raw = raw.shape[0]
    rows = part[0].shape[3]
    step = {d: tuple(lax.rem(me[d] + k, 4) for k in range(4)) for d in "xyz"}

    def device(d, k):
        at = dict(me)
        at[d] = step[d][k]
        return (at["z"], lax.div(at["y"], 2), at["x"], lax.rem(at["y"], 2), c)

    partner = (z, yh, x, yl, 1 - c)

    def slot_at(slot):
        return lax.rem(x + 2 + lax.div(slot, 2), 4), lax.rem(yl + lax.rem(slot, 2), 2)

    raws = (gate_pre, up_pre, hidden_grad)

    def pieces(core):
        found = {}
        for j in range(n_raw):
            for i, ref in enumerate(raws):
                found[("raw", j, i)] = (ref.at[:, pl.ds(j * RAW, RAW)], lambda r, j=j, i=i: raw.at[j, i, r])
        lanes = tile // 4
        for s in range(n_slot):
            sx, sl = slot_at(s)
            at = (sx * 4 + sl * 2 + core) * tile
            for k in range(4):
                src = tokens.at[:, pl.ds(pl.multiple_of(at + step["z"][k] * lanes, lanes), lanes)]
                cut = pl.ds(pl.multiple_of(step["z"][k] * lanes, lanes), lanes)
                found[("tok", s, k)] = (src, lambda r, s=s, cut=cut: tok.at[0, s, r, cut])
            src = out_grad.at[:, pl.ds(pl.multiple_of(at, tile), tile)]
            found[("grad", s)] = (src, lambda r, s=s: tok.at[1, s, r])
        return found

    def raw_names(j):
        return [("raw", j, i) for i in range(3)]

    def rest(slots):
        return [("tok", s, k) for s in slots for k in (0, 1, 3)]

    def grad_names(slots):
        return [("grad", s) for s in slots]

    def lanes_of(slots):
        return lambda r: tok.at[0, pl.ds(0, len(slots)), r, pl.ds(0, 3 * tile // 4)]

    def grads_of(slots):
        return lambda r: tok.at[1, pl.ds(0, len(slots)), r]

    def raw_of(j):
        return lambda r: raw.at[j, :, r]

    far_lanes = pl.ds(pl.multiple_of(step["z"][2] * (tile // 4), tile // 4), tile // 4)
    groups = [(raw_names(0), raw_of(0)),
              ([("tok", s, 2) for s in range(n_slot)], lambda r: tok.at[0, :, r, far_lanes]),
              (rest((0, 1)), lanes_of((0, 1))), (raw_names(1), raw_of(1)),
              (rest((2, 4, 6)), lanes_of((2, 4, 6))), (rest((3, 5, 7)), lanes_of((3, 5, 7)))]
    groups += [(raw_names(j), raw_of(j)) for j in range(2, n_raw)]
    groups += [(grad_names(s), grads_of(s)) for s in ((0, 1), (2, 3, 6, 7), (4, 5))]
    kinds = ("raw", "tok", "grad")
    whole = (lambda r: raw.at[:, :, r], lambda r: tok.at[0, :, r], lambda r: tok.at[1, :, r])
    first_rows, last_rows = pl.ds(0, n_tok), pl.ds(n_tok, n_tok)

    def take(ref, sem):
        pltpu.make_async_copy(ref, ref, sem).wait()

    mine, theirs = pieces(c), pieces(1 - c)
    for names, size in groups:
        for name in names:
            src, dst = mine[name]
            pltpu.make_async_copy(src, dst(first_rows), in_sem.at[kinds.index(name[0])]).start()

    barrier = pltpu.get_barrier_semaphore()
    pl.semaphore_signal(barrier, inc=1, device_id=partner, device_id_type=MESH)
    for d in "xyz":
        for k in (1, 2, 3):
            pl.semaphore_signal(barrier, inc=1, device_id=device(d, k), device_id_type=MESH)
    pl.semaphore_wait(barrier, 10)

    group_of = {}
    for n, (names, size) in enumerate(groups):
        for name in names:
            group_of[name] = n
            src, dst = theirs[name]
            pltpu.make_async_remote_copy(
                src, dst(last_rows), xs_sem.at[kinds.index(name[0])], xr_sem.at[n],
                device_id=partner, device_id_type=MESH).start()

    have = set()

    def need(name):
        kind = kinds.index(name[0])
        if name[0] not in have:
            have.add(name[0])
            take(whole[kind](first_rows), in_sem.at[kind])
        n = group_of[name]
        if n not in have:
            have.add(n)
            take(groups[n][1](last_rows), xr_sem.at[n])

    def hidden(j):
        if ("hidden", j) in have:
            return
        have.add(("hidden", j))
        for i in range(3):
            need(("raw", j, i))

        def body(i, carry):
            at = pl.ds(pl.multiple_of(i * PIECE, PIECE), PIECE)
            cs = pl.ds(j * RAW, RAW)
            gate_val = raw[j, 0, at].astype(F32)
            up_val = raw[j, 1, at].astype(F32)
            grad_val = raw[j, 2, at].astype(F32)
            sig = jax.nn.sigmoid(gate_val)
            activated = gate_val * sig
            hb[2, at, cs] = (activated * up_val).astype(BF16)
            hb[1, at, cs] = (grad_val * activated).astype(BF16)
            hb[0, at, cs] = (grad_val * up_val * sig * (1.0 + gate_val * (1.0 - sig))).astype(BF16)
            return carry

        lax.fori_loop(0, 2 * n_tok // PIECE, body, 0)

    def base(k, ph):
        ref = part[k]
        for d in CHUNKS[k][3][:ph]:
            ref = ref.at[me[d]]
        return ref

    def half_of(ref, i, h):
        n = ref.shape[1] // 2
        return ref.at[i, pl.ds(h * n, n)]

    def send(k, ph, i, src, direction):
        late = 1 if i > 1 or (k, ph) in DIRECT else 0
        pltpu.make_async_remote_copy(
            src, recv[ph][k].at[i], send_sem.at[k, ph], recv_sem.at[k, ph, late],
            device_id=device(CHUNKS[k][3][ph], direction), device_id_type=MESH).start()

    def launch(k, ph, near_side):
        s = step[CHUNKS[k][3][ph]]
        b = base(k, ph)
        if (k, ph) in DIRECT:
            for i, to in ((1, 1), (2, 3)) if near_side else ((0, 2),):
                send(k, ph, i, b.at[s[to]], to)
        elif near_side:
            send(k, ph, 2, half_of(b, s[1], 1), 1)
            send(k, ph, 3, half_of(b, s[3], 0), 3)
        else:
            send(k, ph, 0, half_of(b, s[2], 0), 1)
            send(k, ph, 1, half_of(b, s[2], 1), 3)

    slots_of = (((0, 1), (2, 3, 6, 7), (4, 5)), ((0, 2, 4, 6), (1, 3, 5, 7)), (range(8),) * 3)
    pairs_of = (
        ((1, lambda i: (0, 1)), (2, lambda i: (2 + 4 * i, 3 + 4 * i)), (1, lambda i: (4, 5))),
        ((2, lambda i: (4 * i, 4 * i + 2)), (2, lambda i: (4 * i + 1, 4 * i + 3))),
    )
    z_of = ((1, lambda i: 2), (2, lambda i: 1 + 2 * i), (1, lambda i: 0))

    def multiply(b, seg):
        p, first, dim, widths = BLOCKS[b]
        dim %= 3
        w = p // 2
        for j in range(first // RAW, (first + sum(widths) - 1) // RAW + 1):
            hidden(j)
        for s in slots_of[dim][seg]:
            if w:
                need(("grad", s))
            else:
                for k in ((2,), (1, 3), (0,))[seg] if dim == 2 else range(4):
                    need(("tok", s, k))
        count, which = (z_of if dim == 2 else pairs_of[dim])[seg]
        lanes = tile // 4

        def body(i, carry):
            if dim == 2:
                sz = lax.rem(z + which(i), 4)
                slots, levels = range(n_slot), (sz,)
                cut = pl.ds(pl.multiple_of(sz * lanes, lanes), lanes)
                left = [tok[w, s, :, cut] for s in slots]
            else:
                slots, levels = which(i), range(4)
                left = [tok[w, s] for s in slots]
            res = lax.dot_general(
                jnp.concatenate(left, axis=1), hb[p, :, pl.ds(first, sum(widths))], (((0,), (0,)), ((), ())),
                preferred_element_type=F32).astype(BF16)
            lo = 0
            for slot in slots:
                sx, sl = slot_at(slot)
                for sz in levels:
                    for sh in range(2):
                        at = {"x": sx, "y": sh * 2 + sl, "z": sz}
                        for k in BLOCK_CHUNKS[b]:
                            lane = CHUNKS[k][1] - first
                            o = CHUNKS[k][3]
                            part[k][at[o[0]], at[o[1]], at[o[2]]] = res[lo:lo + rows, lane:lane + CHUNKS[k][2]]
                        lo += rows
            return carry

        lax.fori_loop(0, count, body, 0)

    def add(first, others, dst):
        lead = dst.shape[:-2]
        count = 1
        for n in lead:
            count *= n

        def block(ix):
            v = first[ix].astype(F32)
            for o in others:
                v = v + o[ix].astype(F32)
            dst[ix] = v.astype(dst.dtype)

        if not lead:
            block((slice(None), slice(None)))
            return

        def body(i, carry):
            block((i,) if len(lead) == 1 else (lax.div(i, lead[1]), lax.rem(i, lead[1])))
            return carry

        lax.fori_loop(0, count, body, 0)

    def relay(k, ph):
        s = step[CHUNKS[k][3][ph]]
        take(recv[ph][k].at[pl.ds(0, 2)], recv_sem.at[k, ph, 0])
        for i, to in ((0, 1), (1, 3)):
            got = recv[ph][k].at[i]
            add(got, (half_of(base(k, ph), s[to], i),), got)
            send(k, ph, 4 + i, got, to)

    def finish(k, ph):
        p, first, width, o = CHUNKS[k]
        b, got, at = base(k, ph), recv[ph][k], me[o[ph]]
        cut = pl.ds(first, width)
        if (k, ph) in DIRECT:
            take(got, recv_sem.at[k, ph, 1])
            add(b.at[at], tuple(got.at[i] for i in range(3)), b.at[at] if ph < 2 else result.at[p, :, cut])
        else:
            take(got.at[pl.ds(2, 4)], recv_sem.at[k, ph, 1])
            for h, pair in enumerate(((3, 4), (2, 5))):
                own_half = half_of(b, at, h)
                n = rows // 2
                dst = own_half if ph < 2 else result.at[p, pl.ds(h * n, n), cut]
                add(own_half, tuple(got.at[i] for i in pair), dst)
        if ph == 2:
            pltpu.make_async_copy(result.at[p, :, cut], outs[p].at[:, cut], out_sem.at[0]).start()

    for op, n, m, *h in ORDER:
        (multiply, relay, finish, launch)[op](n, m, *h)

    for kind in range(3):
        take(whole[kind](first_rows), xs_sem.at[kind])
    for k in range(n_chunk):
        ref = part[k]
        for ph in range(3):
            take(ref.at[pl.ds(0, 3)], send_sem.at[k, ph])
            ref = ref.at[0]
    take(result, out_sem.at[0])


def hand_out(*refs):
    held, sem = refs[6:]
    into = [pltpu.make_async_copy(refs[p], held.at[p], sem.at[0, p]) for p in range(3)]
    back = [pltpu.make_async_copy(held.at[p], refs[3 + p], sem.at[1, p]) for p in range(3)]
    for cp in into:
        cp.start()
    for a, b in zip(into, back):
        a.wait()
        b.start()
    for cp in back:
        cp.wait()


def on_device(tokens, out_grad, gate_pre, up_pre, hidden_grad):
    n_tok, width = tokens.shape
    hid = gate_pre.shape[1]
    rows = width // 128
    tile = width // 16
    dma = pltpu.SemaphoreType.DMA
    any_spec = pl.BlockSpec(memory_space=pl.ANY)
    out = jax.ShapeDtypeStruct((rows, hid), F32)
    widths = [k[2] for k in CHUNKS]
    sums = pl.pallas_call(
        kernel,
        out_shape=(out,) * 3,
        in_specs=[any_spec] * 5,
        out_specs=(any_spec,) * 3,
        scratch_shapes=[
            pltpu.VMEM((2, 8, 2 * n_tok, tile), BF16),
            pltpu.VMEM((hid // RAW, 3, 2 * n_tok, RAW), BF16),
            pltpu.VMEM((3, 2 * n_tok, hid), BF16),
            *[pltpu.VMEM((4, 4, 4, rows, w), BF16) for w in widths],
            *[pltpu.VMEM((6, 2, 4, rows, w), BF16) for w in widths],
            *[pltpu.VMEM((3, 4, rows, w) if (k, 1) in DIRECT else (6, 2, rows, w), BF16) for k, w in enumerate(widths)],
            *[pltpu.VMEM((3, rows, w) if (k, 2) in DIRECT else (6, rows // 2, w), BF16) for k, w in enumerate(widths)],
            dma((len(CHUNKS), 3)),
            dma((len(CHUNKS), 3, 2)),
            dma((3,)),
            dma((3,)),
            dma((hid // RAW + 7,)),
            dma((1,)),
            pltpu.VMEM((3, rows, hid), F32),
        ],
        compiler_params=pltpu.CompilerParams(
            collective_id=0, has_side_effects=True, vmem_limit_bytes=67043328),
        name="grad_sum",
    )(tokens, out_grad, gate_pre, up_pre, hidden_grad)
    return pl.pallas_call(
        hand_out, out_shape=(out,) * 3, in_specs=[any_spec] * 3, out_specs=(any_spec,) * 3,
        scratch_shapes=[pltpu.VMEM((3, rows, hid), F32), dma((2, 3))], name="hand_out")(*sums)


def solution(mesh):
    split = Mesh(mesh.devices.reshape(4, 2, 4, 2, 2), AXES)
    spec_in = P(AXES, None)
    spec_out = P(("x", "yl", "c", "z", "yh"), None)
    return jax.shard_map(
        on_device, mesh=split, in_specs=(spec_in,) * 5, out_specs=(spec_out,) * 3, check_vma=False
    )
```

```python
import jax
import jax.numpy as jnp
from jax import lax
from jax.experimental import pallas as pl
from jax.experimental.pallas import tpu as pltpu
from jax.sharding import Mesh
from jax.sharding import PartitionSpec as P

AXES = ("z", "yh", "x", "yl", "c")
DIM_ORDERS = ("xyz", "yzx", "zxy", "xzy", "yxz", "zyx")
MESH = pl.DeviceIdType.MESH
F32, BF16 = jnp.float32, jnp.bfloat16

BLOCKS = (
    (0, 0, (2,), (256,)),
    (1, 0, (0,), (256,)),
    (0, 256, (1,), (256,)),
    (1, 256, (2,), (256,)),
    (0, 512, (0, 3), (128, 128)),
    (1, 512, (1,), (256,)),
    (2, 0, (2,), (256,)),
    (2, 256, (0,), (256,)),
    (2, 512, (1,), (256,)),
)
ORDER = (
    (0, 0, 0), (3, 0, 0, 0), (0, 1, 0), (3, 1, 0, 0), (0, 3, 0), (3, 3, 0, 0), (0, 2, 0), (3, 2, 0, 0),
    (0, 4, 0), (3, 5, 0, 0), (0, 4, 1), (0, 2, 1), (3, 4, 0, 1), (0, 0, 1), (3, 0, 0, 1), (3, 4, 0, 0),
    (3, 2, 0, 1), (0, 8, 0), (0, 1, 1), (0, 3, 1), (1, 5, 0), (0, 6, 0), (1, 0, 0), (3, 9, 0, 0),
    (0, 7, 0), (3, 7, 0, 0), (0, 8, 1), (3, 8, 0, 0), (1, 3, 0), (3, 9, 0, 1), (0, 0, 2), (0, 6, 1),
    (0, 7, 1), (3, 5, 0, 1), (1, 4, 0), (0, 4, 2), (0, 5, 0), (3, 1, 0, 1), (1, 2, 0), (0, 3, 2),
    (1, 8, 0), (0, 1, 2), (3, 6, 0, 0), (1, 9, 0), (3, 8, 0, 1), (2, 0, 0), (0, 5, 1), (3, 7, 0, 1),
    (0, 7, 2), (2, 5, 0), (3, 5, 1, 0), (3, 3, 0, 1), (1, 1, 0), (1, 6, 0), (2, 4, 0), (3, 0, 1, 0),
    (1, 7, 0), (3, 6, 0, 1), (0, 6, 2), (3, 4, 1, 0), (2, 3, 0), (2, 9, 0), (3, 3, 1, 0), (2, 2, 0),
    (3, 2, 1, 0), (3, 4, 1, 1), (3, 3, 1, 1), (3, 9, 1, 1), (2, 8, 0), (3, 9, 1, 0), (2, 7, 0), (3, 7, 1, 0),
    (3, 2, 1, 1), (2, 1, 0), (1, 5, 1), (3, 0, 1, 1), (3, 1, 1, 0), (3, 8, 1, 0), (2, 6, 0), (3, 6, 1, 0),
    (3, 5, 1, 1), (3, 1, 1, 1), (1, 4, 1), (1, 2, 1), (1, 0, 1), (1, 9, 1), (1, 3, 1), (1, 7, 1),
    (1, 1, 1), (3, 8, 1, 1), (3, 6, 1, 1), (3, 7, 1, 1), (2, 0, 1), (1, 8, 1), (2, 4, 1), (3, 0, 2, 0),
    (3, 4, 2, 0), (1, 6, 1), (3, 0, 2, 1), (2, 2, 1), (3, 2, 2, 0), (2, 3, 1), (2, 5, 1), (2, 9, 1),
    (3, 5, 2, 0), (3, 3, 2, 0), (3, 4, 2, 1), (3, 9, 2, 1), (3, 3, 2, 1), (3, 9, 2, 0), (2, 1, 1), (3, 1, 2, 0),
    (3, 5, 2, 1), (2, 7, 1), (3, 7, 2, 0), (3, 1, 2, 1), (1, 4, 2), (1, 2, 2), (2, 8, 1), (3, 2, 2, 1),
    (3, 8, 2, 0), (1, 0, 2), (3, 7, 2, 1), (2, 6, 1), (3, 6, 2, 0), (1, 1, 2), (3, 6, 2, 1), (3, 8, 2, 1),
    (1, 5, 2), (1, 3, 2), (2, 4, 2), (2, 0, 2), (2, 9, 2), (2, 2, 2), (2, 1, 2), (2, 5, 2),
    (2, 7, 2), (2, 3, 2), (2, 8, 2), (2, 6, 2),
)
DIRECT = ((6, 2), (7, 2), (8, 2), (9, 2))
CHUNKS = tuple(
    (b[0], b[1] + sum(b[3][:i]), w, DIM_ORDERS[b[2][i]]) for b in BLOCKS for i, w in enumerate(b[3]))
BLOCK_CHUNKS = tuple(
    tuple(sum(len(a[3]) for a in BLOCKS[:n]) + i for i in range(len(b[3]))) for n, b in enumerate(BLOCKS))
RAW = 256
PIECE = 64


def kernel(*refs):
    tokens, out_grad, gate_pre, up_pre, hidden_grad = refs[:5]
    outs = refs[5:8]
    tok, raw, hb = refs[8:11]
    n_chunk = len(CHUNKS)
    part = refs[11:11 + n_chunk]
    recv = tuple(refs[11 + (1 + ph) * n_chunk:11 + (2 + ph) * n_chunk] for ph in range(3))
    send_sem, recv_sem, in_sem, xs_sem, xr_sem, out_sem, result = refs[11 + 4 * n_chunk:]

    z, yh, x, yl, c = (lax.axis_index(a) for a in AXES)
    y = yh * 2 + yl
    me = {"x": x, "y": y, "z": z}
    n_tok = tokens.shape[0]
    n_slot, tile = tok.shape[1], tok.shape[3]
    n_raw = raw.shape[0]
    rows = part[0].shape[3]
    step = {d: tuple(lax.rem(me[d] + k, 4) for k in range(4)) for d in "xyz"}

    def device(d, k):
        at = dict(me)
        at[d] = step[d][k]
        return (at["z"], lax.div(at["y"], 2), at["x"], lax.rem(at["y"], 2), c)

    partner = (z, yh, x, yl, 1 - c)

    def slot_at(slot):
        return lax.rem(x + 2 + lax.div(slot, 2), 4), lax.rem(yl + lax.rem(slot, 2), 2)

    raws = (gate_pre, up_pre, hidden_grad)

    def pieces(core):
        found = {}
        for j in range(n_raw):
            for i, ref in enumerate(raws):
                found[("raw", j, i)] = (ref.at[:, pl.ds(j * RAW, RAW)], lambda r, j=j, i=i: raw.at[j, i, r])
        lanes = tile // 4
        for s in range(n_slot):
            sx, sl = slot_at(s)
            at = (sx * 4 + sl * 2 + core) * tile
            for k in range(4):
                src = tokens.at[:, pl.ds(pl.multiple_of(at + step["z"][k] * lanes, lanes), lanes)]
                cut = pl.ds(pl.multiple_of(step["z"][k] * lanes, lanes), lanes)
                found[("tok", s, k)] = (src, lambda r, s=s, cut=cut: tok.at[0, s, r, cut])
            src = out_grad.at[:, pl.ds(pl.multiple_of(at, tile), tile)]
            found[("grad", s)] = (src, lambda r, s=s: tok.at[1, s, r])
        return found

    def raw_names(j):
        return [("raw", j, i) for i in range(3)]

    def rest(slots):
        return [("tok", s, k) for s in slots for k in (0, 1, 3)]

    def grad_names(slots):
        return [("grad", s) for s in slots]

    def lanes_of(slots):
        return lambda r: tok.at[0, pl.ds(0, len(slots)), r, pl.ds(0, 3 * tile // 4)]

    def grads_of(slots):
        return lambda r: tok.at[1, pl.ds(0, len(slots)), r]

    def raw_of(j):
        return lambda r: raw.at[j, :, r]

    far_lanes = pl.ds(pl.multiple_of(step["z"][2] * (tile // 4), tile // 4), tile // 4)
    groups = [(raw_names(0), raw_of(0)),
              ([("tok", s, 2) for s in range(n_slot)], lambda r: tok.at[0, :, r, far_lanes]),
              (rest((0, 1)), lanes_of((0, 1))), (raw_names(1), raw_of(1)),
              (rest((2, 4, 6)), lanes_of((2, 4, 6))), (rest((3, 5, 7)), lanes_of((3, 5, 7)))]
    groups += [(raw_names(j), raw_of(j)) for j in range(2, n_raw)]
    groups += [(grad_names(s), grads_of(s)) for s in ((0, 1), (2, 3, 6, 7), (4, 5))]
    kinds = ("raw", "tok", "grad")
    whole = (lambda r: raw.at[:, :, r], lambda r: tok.at[0, :, r], lambda r: tok.at[1, :, r])
    first_rows, last_rows = pl.ds(0, n_tok), pl.ds(n_tok, n_tok)

    def take(ref, sem):
        pltpu.make_async_copy(ref, ref, sem).wait()

    mine, theirs = pieces(c), pieces(1 - c)
    for names, size in groups:
        for name in names:
            src, dst = mine[name]
            pltpu.make_async_copy(src, dst(first_rows), in_sem.at[kinds.index(name[0])]).start()

    barrier = pltpu.get_barrier_semaphore()
    pl.semaphore_signal(barrier, inc=1, device_id=partner, device_id_type=MESH)
    for d in "xyz":
        for k in (1, 2, 3):
            pl.semaphore_signal(barrier, inc=1, device_id=device(d, k), device_id_type=MESH)
    pl.semaphore_wait(barrier, 10)

    group_of = {}
    for n, (names, size) in enumerate(groups):
        for name in names:
            group_of[name] = n
            src, dst = theirs[name]
            pltpu.make_async_remote_copy(
                src, dst(last_rows), xs_sem.at[kinds.index(name[0])], xr_sem.at[n],
                device_id=partner, device_id_type=MESH).start()

    have = set()

    def need(name):
        kind = kinds.index(name[0])
        if name[0] not in have:
            have.add(name[0])
            take(whole[kind](first_rows), in_sem.at[kind])
        n = group_of[name]
        if n not in have:
            have.add(n)
            take(groups[n][1](last_rows), xr_sem.at[n])

    def hidden(j):
        if ("hidden", j) in have:
            return
        have.add(("hidden", j))
        for i in range(3):
            need(("raw", j, i))

        def body(i, carry):
            at = pl.ds(pl.multiple_of(i * PIECE, PIECE), PIECE)
            cs = pl.ds(j * RAW, RAW)
            gate_val = raw[j, 0, at].astype(F32)
            up_val = raw[j, 1, at].astype(F32)
            grad_val = raw[j, 2, at].astype(F32)
            sig = jax.nn.sigmoid(gate_val)
            activated = gate_val * sig
            hb[2, at, cs] = (activated * up_val).astype(BF16)
            hb[1, at, cs] = (grad_val * activated).astype(BF16)
            hb[0, at, cs] = (grad_val * up_val * sig * (1.0 + gate_val * (1.0 - sig))).astype(BF16)
            return carry

        lax.fori_loop(0, 2 * n_tok // PIECE, body, 0)

    def base(k, ph):
        ref = part[k]
        for d in CHUNKS[k][3][:ph]:
            ref = ref.at[me[d]]
        return ref

    def half_of(ref, i, h):
        n = ref.shape[1] // 2
        return ref.at[i, pl.ds(h * n, n)]

    def send(k, ph, i, src, direction):
        late = 1 if i > 1 or (k, ph) in DIRECT else 0
        pltpu.make_async_remote_copy(
            src, recv[ph][k].at[i], send_sem.at[k, ph], recv_sem.at[k, ph, late],
            device_id=device(CHUNKS[k][3][ph], direction), device_id_type=MESH).start()

    def launch(k, ph, near_side):
        s = step[CHUNKS[k][3][ph]]
        b = base(k, ph)
        if (k, ph) in DIRECT:
            for i, to in ((1, 1), (2, 3)) if near_side else ((0, 2),):
                send(k, ph, i, b.at[s[to]], to)
        elif near_side:
            send(k, ph, 2, half_of(b, s[1], 1), 1)
            send(k, ph, 3, half_of(b, s[3], 0), 3)
        else:
            send(k, ph, 0, half_of(b, s[2], 0), 1)
            send(k, ph, 1, half_of(b, s[2], 1), 3)

    slots_of = (((0, 1), (2, 3, 6, 7), (4, 5)), ((0, 2, 4, 6), (1, 3, 5, 7)), (range(8),) * 3)
    pairs_of = (
        ((1, lambda i: (0, 1)), (2, lambda i: (2 + 4 * i, 3 + 4 * i)), (1, lambda i: (4, 5))),
        ((2, lambda i: (4 * i, 4 * i + 2)), (2, lambda i: (4 * i + 1, 4 * i + 3))),
    )
    z_of = ((1, lambda i: 2), (2, lambda i: 1 + 2 * i), (1, lambda i: 0))

    def multiply(b, seg):
        p, first, dim, widths = BLOCKS[b]
        dim = dim[0] % 3
        w = p // 2
        for j in range(first // RAW, (first + sum(widths) - 1) // RAW + 1):
            hidden(j)
        for s in slots_of[dim][seg]:
            if w:
                need(("grad", s))
            else:
                for k in ((2,), (1, 3), (0,))[seg] if dim == 2 else range(4):
                    need(("tok", s, k))
        count, which = (z_of if dim == 2 else pairs_of[dim])[seg]
        lanes = tile // 4

        def body(i, carry):
            if dim == 2:
                sz = lax.rem(z + which(i), 4)
                slots, levels = range(n_slot), (sz,)
                cut = pl.ds(pl.multiple_of(sz * lanes, lanes), lanes)
                left = [tok[w, s, :, cut] for s in slots]
            else:
                slots, levels = which(i), range(4)
                left = [tok[w, s] for s in slots]
            res = lax.dot_general(
                jnp.concatenate(left, axis=1), hb[p, :, pl.ds(first, sum(widths))], (((0,), (0,)), ((), ())),
                preferred_element_type=F32).astype(BF16)
            lo = 0
            for slot in slots:
                sx, sl = slot_at(slot)
                for sz in levels:
                    for sh in range(2):
                        at = {"x": sx, "y": sh * 2 + sl, "z": sz}
                        for k in BLOCK_CHUNKS[b]:
                            lane = CHUNKS[k][1] - first
                            o = CHUNKS[k][3]
                            part[k][at[o[0]], at[o[1]], at[o[2]]] = res[lo:lo + rows, lane:lane + CHUNKS[k][2]]
                        lo += rows
            return carry

        lax.fori_loop(0, count, body, 0)

    def add(first, others, dst):
        lead = dst.shape[:-2]
        count = 1
        for n in lead:
            count *= n

        def block(ix):
            v = first[ix].astype(F32)
            for o in others:
                v = v + o[ix].astype(F32)
            dst[ix] = v.astype(dst.dtype)

        if not lead:
            block((slice(None), slice(None)))
            return

        def body(i, carry):
            block((i,) if len(lead) == 1 else (lax.div(i, lead[1]), lax.rem(i, lead[1])))
            return carry

        lax.fori_loop(0, count, body, 0)

    def relay(k, ph):
        s = step[CHUNKS[k][3][ph]]
        take(recv[ph][k].at[pl.ds(0, 2)], recv_sem.at[k, ph, 0])
        for i, to in ((0, 1), (1, 3)):
            got = recv[ph][k].at[i]
            add(got, (half_of(base(k, ph), s[to], i),), got)
            send(k, ph, 4 + i, got, to)

    def finish(k, ph):
        p, first, width, o = CHUNKS[k]
        b, got, at = base(k, ph), recv[ph][k], me[o[ph]]
        cut = pl.ds(first, width)
        if (k, ph) in DIRECT:
            take(got, recv_sem.at[k, ph, 1])
            add(b.at[at], tuple(got.at[i] for i in range(3)), b.at[at] if ph < 2 else result.at[p, :, cut])
        else:
            take(got.at[pl.ds(2, 4)], recv_sem.at[k, ph, 1])
            for h, pair in enumerate(((3, 4), (2, 5))):
                own_half = half_of(b, at, h)
                n = rows // 2
                dst = own_half if ph < 2 else result.at[p, pl.ds(h * n, n), cut]
                add(own_half, tuple(got.at[i] for i in pair), dst)
        if ph == 2:
            pltpu.make_async_copy(result.at[p, :, cut], outs[p].at[:, cut], out_sem.at[0]).start()

    for op, n, m, *h in ORDER:
        (multiply, relay, finish, launch)[op](n, m, *h)

    for kind in range(3):
        take(whole[kind](first_rows), xs_sem.at[kind])
    for k in range(n_chunk):
        ref = part[k]
        for ph in range(3):
            take(ref.at[pl.ds(0, 3)], send_sem.at[k, ph])
            ref = ref.at[0]
    take(result, out_sem.at[0])


def hand_out(*refs):
    held, sem = refs[6:]
    into = [pltpu.make_async_copy(refs[p], held.at[p], sem.at[0, p]) for p in range(3)]
    back = [pltpu.make_async_copy(held.at[p], refs[3 + p], sem.at[1, p]) for p in range(3)]
    for cp in into:
        cp.start()
    for a, b in zip(into, back):
        a.wait()
        b.start()
    for cp in back:
        cp.wait()


def on_device(tokens, out_grad, gate_pre, up_pre, hidden_grad):
    n_tok, width = tokens.shape
    hid = gate_pre.shape[1]
    rows = width // 128
    tile = width // 16
    dma = pltpu.SemaphoreType.DMA
    any_spec = pl.BlockSpec(memory_space=pl.ANY)
    out = jax.ShapeDtypeStruct((rows, hid), F32)
    widths = [k[2] for k in CHUNKS]
    sums = pl.pallas_call(
        kernel,
        out_shape=(out,) * 3,
        in_specs=[any_spec] * 5,
        out_specs=(any_spec,) * 3,
        scratch_shapes=[
            pltpu.VMEM((2, 8, 2 * n_tok, tile), BF16),
            pltpu.VMEM((hid // RAW, 3, 2 * n_tok, RAW), BF16),
            pltpu.VMEM((3, 2 * n_tok, hid), BF16),
            *[pltpu.VMEM((4, 4, 4, rows, w), BF16) for w in widths],
            *[pltpu.VMEM((6, 2, 4, rows, w), BF16) for w in widths],
            *[pltpu.VMEM((3, 4, rows, w) if (k, 1) in DIRECT else (6, 2, rows, w), BF16) for k, w in enumerate(widths)],
            *[pltpu.VMEM((3, rows, w) if (k, 2) in DIRECT else (6, rows // 2, w), BF16) for k, w in enumerate(widths)],
            dma((len(CHUNKS), 3)),
            dma((len(CHUNKS), 3, 2)),
            dma((3,)),
            dma((3,)),
            dma((hid // RAW + 7,)),
            dma((1,)),
            pltpu.VMEM((3, rows, hid), F32),
        ],
        compiler_params=pltpu.CompilerParams(
            collective_id=0, has_side_effects=True, vmem_limit_bytes=67043328),
        name="grad_sum",
    )(tokens, out_grad, gate_pre, up_pre, hidden_grad)
    return pl.pallas_call(
        hand_out, out_shape=(out,) * 3, in_specs=[any_spec] * 3, out_specs=(any_spec,) * 3,
        scratch_shapes=[pltpu.VMEM((3, rows, hid), F32), dma((2, 3))], name="hand_out")(*sums)


def solution(mesh):
    split = Mesh(mesh.devices.reshape(4, 2, 4, 2, 2), AXES)
    spec_in = P(AXES, None)
    spec_out = P(("x", "yl", "c", "z", "yh"), None)
    return jax.shard_map(
        on_device, mesh=split, in_specs=(spec_in,) * 5, out_specs=(spec_out,) * 3, check_vma=False
    )
```

```python
import jax
import jax.numpy as jnp
from jax import lax
from jax.experimental import pallas as pl
from jax.experimental.pallas import tpu as pltpu
from jax.sharding import Mesh
from jax.sharding import PartitionSpec as P

AXES = ("z", "yh", "x", "yl", "c")
DIM_ORDERS = ("xyz", "yzx", "zxy", "xzy", "yxz", "zyx")
MESH = pl.DeviceIdType.MESH
F32, BF16 = jnp.float32, jnp.bfloat16

BLOCKS = (
    (0, 0, (2,), (256,)),
    (1, 0, (0,), (256,)),
    (0, 256, (1,), (256,)),
    (1, 256, (2,), (256,)),
    (0, 512, (0, 3), (128, 128)),
    (1, 512, (1,), (256,)),
    (2, 0, (2,), (256,)),
    (2, 256, (0,), (256,)),
    (2, 512, (1,), (256,)),
)
ORDER = (
    (0, 0, 0), (3, 0, 0, 0), (0, 1, 0), (3, 1, 0, 0), (0, 3, 0), (3, 3, 0, 0), (0, 2, 0), (3, 2, 0, 0),
    (0, 4, 0), (3, 5, 0, 0), (0, 4, 1), (0, 2, 1), (3, 4, 0, 1), (0, 0, 1), (3, 0, 0, 1), (3, 4, 0, 0),
    (3, 2, 0, 1), (0, 8, 0), (0, 1, 1), (0, 3, 1), (1, 5, 0), (0, 6, 0), (1, 0, 0), (3, 9, 0, 0),
    (0, 7, 0), (3, 7, 0, 0), (0, 8, 1), (3, 8, 0, 0), (1, 3, 0), (3, 9, 0, 1), (0, 0, 2), (0, 6, 1),
    (0, 7, 1), (3, 5, 0, 1), (1, 4, 0), (0, 4, 2), (0, 5, 0), (3, 1, 0, 1), (1, 2, 0), (0, 3, 2),
    (1, 8, 0), (0, 1, 2), (3, 6, 0, 0), (1, 9, 0), (3, 8, 0, 1), (2, 0, 0), (0, 5, 1), (3, 7, 0, 1),
    (0, 7, 2), (2, 5, 0), (3, 5, 1, 0), (3, 3, 0, 1), (1, 1, 0), (1, 6, 0), (2, 4, 0), (3, 0, 1, 0),
    (1, 7, 0), (3, 6, 0, 1), (0, 6, 2), (3, 4, 1, 0), (2, 3, 0), (2, 9, 0), (3, 3, 1, 0), (2, 2, 0),
    (3, 2, 1, 0), (3, 4, 1, 1), (3, 3, 1, 1), (3, 9, 1, 1), (2, 8, 0), (3, 9, 1, 0), (2, 7, 0), (3, 7, 1, 0),
    (3, 2, 1, 1), (2, 1, 0), (1, 5, 1), (3, 0, 1, 1), (3, 1, 1, 0), (3, 8, 1, 0), (2, 6, 0), (3, 6, 1, 0),
    (3, 5, 1, 1), (3, 1, 1, 1), (1, 4, 1), (1, 2, 1), (1, 0, 1), (1, 9, 1), (1, 3, 1), (1, 7, 1),
    (1, 1, 1), (3, 8, 1, 1), (3, 6, 1, 1), (3, 7, 1, 1), (2, 0, 1), (1, 8, 1), (2, 4, 1), (3, 0, 2, 0),
    (3, 4, 2, 0), (1, 6, 1), (3, 0, 2, 1), (2, 2, 1), (3, 2, 2, 0), (2, 3, 1), (2, 5, 1), (2, 9, 1),
    (3, 5, 2, 0), (3, 3, 2, 0), (3, 4, 2, 1), (3, 9, 2, 1), (3, 3, 2, 1), (3, 9, 2, 0), (2, 1, 1), (3, 1, 2, 0),
    (3, 5, 2, 1), (2, 7, 1), (3, 7, 2, 0), (3, 1, 2, 1), (1, 4, 2), (1, 2, 2), (2, 8, 1), (3, 2, 2, 1),
    (3, 8, 2, 0), (1, 0, 2), (3, 7, 2, 1), (2, 6, 1), (3, 6, 2, 0), (1, 1, 2), (3, 6, 2, 1), (3, 8, 2, 1),
    (1, 5, 2), (1, 3, 2), (2, 4, 2), (2, 0, 2), (2, 9, 2), (2, 2, 2), (2, 1, 2), (2, 5, 2),
    (2, 7, 2), (2, 3, 2), (2, 8, 2), (2, 6, 2),
)
DIRECT = ((6, 2), (7, 2), (8, 2), (9, 2))
CHUNKS = tuple(
    (b[0], b[1] + sum(b[3][:i]), w, DIM_ORDERS[b[2][i]]) for b in BLOCKS for i, w in enumerate(b[3]))
BLOCK_CHUNKS = tuple(
    tuple(sum(len(a[3]) for a in BLOCKS[:n]) + i for i in range(len(b[3]))) for n, b in enumerate(BLOCKS))
RAW = 256
PIECE = 64


def kernel(*refs):
    tokens, out_grad, gate_pre, up_pre, hidden_grad = refs[:5]
    outs = refs[5:8]
    tok, raw, hb = refs[8:11]
    n_chunk = len(CHUNKS)
    part = refs[11:11 + n_chunk]
    recv = tuple(refs[11 + (1 + ph) * n_chunk:11 + (2 + ph) * n_chunk] for ph in range(3))
    send_sem, recv_sem, in_sem, xs_sem, xr_sem = refs[11 + 4 * n_chunk:]

    z, yh, x, yl, c = (lax.axis_index(a) for a in AXES)
    y = yh * 2 + yl
    me = {"x": x, "y": y, "z": z}
    n_tok = tokens.shape[0]
    n_slot, tile = tok.shape[1], tok.shape[3]
    n_raw = raw.shape[0]
    rows = part[0].shape[3]
    step = {d: tuple(lax.rem(me[d] + k, 4) for k in range(4)) for d in "xyz"}

    def device(d, k):
        at = dict(me)
        at[d] = step[d][k]
        return (at["z"], lax.div(at["y"], 2), at["x"], lax.rem(at["y"], 2), c)

    partner = (z, yh, x, yl, 1 - c)

    def slot_at(slot):
        return lax.rem(x + 2 + lax.div(slot, 2), 4), lax.rem(yl + lax.rem(slot, 2), 2)

    raws = (gate_pre, up_pre, hidden_grad)

    def pieces(core):
        found = {}
        for j in range(n_raw):
            for i, ref in enumerate(raws):
                found[("raw", j, i)] = (ref.at[:, pl.ds(j * RAW, RAW)], lambda r, j=j, i=i: raw.at[j, i, r])
        lanes = tile // 4
        for s in range(n_slot):
            sx, sl = slot_at(s)
            at = (sx * 4 + sl * 2 + core) * tile
            for k in range(4):
                src = tokens.at[:, pl.ds(pl.multiple_of(at + step["z"][k] * lanes, lanes), lanes)]
                cut = pl.ds(pl.multiple_of(step["z"][k] * lanes, lanes), lanes)
                found[("tok", s, k)] = (src, lambda r, s=s, cut=cut: tok.at[0, s, r, cut])
            src = out_grad.at[:, pl.ds(pl.multiple_of(at, tile), tile)]
            found[("grad", s)] = (src, lambda r, s=s: tok.at[1, s, r])
        return found

    def raw_names(j):
        return [("raw", j, i) for i in range(3)]

    def rest(slots):
        return [("tok", s, k) for s in slots for k in (0, 1, 3)]

    def grad_names(slots):
        return [("grad", s) for s in slots]

    def lanes_of(slots):
        return lambda r: tok.at[0, pl.ds(0, len(slots)), r, pl.ds(0, 3 * tile // 4)]

    def grads_of(slots):
        return lambda r: tok.at[1, pl.ds(0, len(slots)), r]

    def raw_of(j):
        return lambda r: raw.at[j, :, r]

    far_lanes = pl.ds(pl.multiple_of(step["z"][2] * (tile // 4), tile // 4), tile // 4)
    groups = [(raw_names(0), raw_of(0)),
              ([("tok", s, 2) for s in range(n_slot)], lambda r: tok.at[0, :, r, far_lanes]),
              (rest((0, 1)), lanes_of((0, 1))), (raw_names(1), raw_of(1)),
              (rest((2, 4, 6)), lanes_of((2, 4, 6))), (rest((3, 5, 7)), lanes_of((3, 5, 7)))]
    groups += [(raw_names(j), raw_of(j)) for j in range(2, n_raw)]
    groups += [(grad_names(s), grads_of(s)) for s in ((0, 1), (2, 3, 6, 7), (4, 5))]
    kinds = ("raw", "tok", "grad")
    whole = (lambda r: raw.at[:, :, r], lambda r: tok.at[0, :, r], lambda r: tok.at[1, :, r])
    first_rows, last_rows = pl.ds(0, n_tok), pl.ds(n_tok, n_tok)

    def take(ref, sem):
        pltpu.make_async_copy(ref, ref, sem).wait()

    mine, theirs = pieces(c), pieces(1 - c)
    for names, size in groups:
        for name in names:
            src, dst = mine[name]
            pltpu.make_async_copy(src, dst(first_rows), in_sem.at[kinds.index(name[0])]).start()

    barrier = pltpu.get_barrier_semaphore()
    pl.semaphore_signal(barrier, inc=1, device_id=partner, device_id_type=MESH)
    for d in "xyz":
        for k in (1, 2, 3):
            pl.semaphore_signal(barrier, inc=1, device_id=device(d, k), device_id_type=MESH)
    pl.semaphore_wait(barrier, 10)

    group_of = {}
    for n, (names, size) in enumerate(groups):
        for name in names:
            group_of[name] = n
            src, dst = theirs[name]
            pltpu.make_async_remote_copy(
                src, dst(last_rows), xs_sem.at[kinds.index(name[0])], xr_sem.at[n],
                device_id=partner, device_id_type=MESH).start()

    have = set()

    def need(name):
        kind = kinds.index(name[0])
        if name[0] not in have:
            have.add(name[0])
            take(whole[kind](first_rows), in_sem.at[kind])
        n = group_of[name]
        if n not in have:
            have.add(n)
            take(groups[n][1](last_rows), xr_sem.at[n])

    def hidden(j):
        if ("hidden", j) in have:
            return
        have.add(("hidden", j))
        for i in range(3):
            need(("raw", j, i))

        def body(i, carry):
            at = pl.ds(pl.multiple_of(i * PIECE, PIECE), PIECE)
            cs = pl.ds(j * RAW, RAW)
            gate_val = raw[j, 0, at].astype(F32)
            up_val = raw[j, 1, at].astype(F32)
            grad_val = raw[j, 2, at].astype(F32)
            sig = jax.nn.sigmoid(gate_val)
            activated = gate_val * sig
            hb[2, at, cs] = (activated * up_val).astype(BF16)
            hb[1, at, cs] = (grad_val * activated).astype(BF16)
            hb[0, at, cs] = (grad_val * up_val * sig * (1.0 + gate_val * (1.0 - sig))).astype(BF16)
            return carry

        lax.fori_loop(0, 2 * n_tok // PIECE, body, 0)

    def base(k, ph):
        ref = part[k]
        for d in CHUNKS[k][3][:ph]:
            ref = ref.at[me[d]]
        return ref

    def half_of(ref, i, h):
        n = ref.shape[1] // 2
        return ref.at[i, pl.ds(h * n, n)]

    def send(k, ph, i, src, direction):
        late = 1 if i > 1 or (k, ph) in DIRECT else 0
        pltpu.make_async_remote_copy(
            src, recv[ph][k].at[i], send_sem.at[k, ph], recv_sem.at[k, ph, late],
            device_id=device(CHUNKS[k][3][ph], direction), device_id_type=MESH).start()

    def launch(k, ph, near_side):
        s = step[CHUNKS[k][3][ph]]
        b = base(k, ph)
        if (k, ph) in DIRECT:
            for i, to in ((1, 1), (2, 3)) if near_side else ((0, 2),):
                send(k, ph, i, b.at[s[to]], to)
        elif near_side:
            send(k, ph, 2, half_of(b, s[1], 1), 1)
            send(k, ph, 3, half_of(b, s[3], 0), 3)
        else:
            send(k, ph, 0, half_of(b, s[2], 0), 1)
            send(k, ph, 1, half_of(b, s[2], 1), 3)

    slots_of = (((0, 1), (2, 3, 6, 7), (4, 5)), ((0, 2, 4, 6), (1, 3, 5, 7)), (range(8),) * 3)
    pairs_of = (
        ((1, lambda i: (0, 1)), (2, lambda i: (2 + 4 * i, 3 + 4 * i)), (1, lambda i: (4, 5))),
        ((2, lambda i: (4 * i, 4 * i + 2)), (2, lambda i: (4 * i + 1, 4 * i + 3))),
    )
    z_of = ((1, lambda i: 2), (2, lambda i: 1 + 2 * i), (1, lambda i: 0))

    def multiply(b, seg):
        p, first, dim, widths = BLOCKS[b]
        dim = dim[0] % 3
        w = p // 2
        for j in range(first // RAW, (first + sum(widths) - 1) // RAW + 1):
            hidden(j)
        for s in slots_of[dim][seg]:
            if w:
                need(("grad", s))
            else:
                for k in ((2,), (1, 3), (0,))[seg] if dim == 2 else range(4):
                    need(("tok", s, k))
        count, which = (z_of if dim == 2 else pairs_of[dim])[seg]
        lanes = tile // 4

        def body(i, carry):
            if dim == 2:
                sz = lax.rem(z + which(i), 4)
                slots, levels = range(n_slot), (sz,)
                cut = pl.ds(pl.multiple_of(sz * lanes, lanes), lanes)
                left = [tok[w, s, :, cut] for s in slots]
            else:
                slots, levels = which(i), range(4)
                left = [tok[w, s] for s in slots]
            res = lax.dot_general(
                jnp.concatenate(left, axis=1), hb[p, :, pl.ds(first, sum(widths))], (((0,), (0,)), ((), ())),
                preferred_element_type=F32).astype(BF16)
            lo = 0
            for slot in slots:
                sx, sl = slot_at(slot)
                for sz in levels:
                    for sh in range(2):
                        at = {"x": sx, "y": sh * 2 + sl, "z": sz}
                        for k in BLOCK_CHUNKS[b]:
                            lane = CHUNKS[k][1] - first
                            o = CHUNKS[k][3]
                            part[k][at[o[0]], at[o[1]], at[o[2]]] = res[lo:lo + rows, lane:lane + CHUNKS[k][2]]
                        lo += rows
            return carry

        lax.fori_loop(0, count, body, 0)

    def add(first, others, dst):
        lead = dst.shape[:-2]
        count = 1
        for n in lead:
            count *= n

        def block(ix):
            v = first[ix].astype(F32)
            for o in others:
                v = v + o[ix].astype(F32)
            dst[ix] = v.astype(dst.dtype)

        if not lead:
            block((slice(None), slice(None)))
            return

        def body(i, carry):
            block((i,) if len(lead) == 1 else (lax.div(i, lead[1]), lax.rem(i, lead[1])))
            return carry

        lax.fori_loop(0, count, body, 0)

    def relay(k, ph):
        s = step[CHUNKS[k][3][ph]]
        take(recv[ph][k].at[pl.ds(0, 2)], recv_sem.at[k, ph, 0])
        for i, to in ((0, 1), (1, 3)):
            got = recv[ph][k].at[i]
            add(got, (half_of(base(k, ph), s[to], i),), got)
            send(k, ph, 4 + i, got, to)

    def finish(k, ph):
        p, first, width, o = CHUNKS[k]
        b, got, at = base(k, ph), recv[ph][k], me[o[ph]]
        cut = pl.ds(first, width)
        if (k, ph) in DIRECT:
            take(got, recv_sem.at[k, ph, 1])
            add(b.at[at], tuple(got.at[i] for i in range(3)), b.at[at] if ph < 2 else outs[p].at[:, cut])
        else:
            take(got.at[pl.ds(2, 4)], recv_sem.at[k, ph, 1])
            for h, pair in enumerate(((3, 4), (2, 5))):
                own_half = half_of(b, at, h)
                n = rows // 2
                dst = own_half if ph < 2 else outs[p].at[pl.ds(h * n, n), cut]
                add(own_half, tuple(got.at[i] for i in pair), dst)

    for op, n, m, *h in ORDER:
        (multiply, relay, finish, launch)[op](n, m, *h)

    for kind in range(3):
        take(whole[kind](first_rows), xs_sem.at[kind])
    for k in range(n_chunk):
        ref = part[k]
        for ph in range(3):
            take(ref.at[pl.ds(0, 3)], send_sem.at[k, ph])
            ref = ref.at[0]


def hand_out(*refs):
    copies = [pltpu.make_async_copy(refs[p], refs[3 + p], refs[6].at[p]) for p in range(3)]
    for cp in copies:
        cp.start()
    for cp in copies:
        cp.wait()


def on_device(tokens, out_grad, gate_pre, up_pre, hidden_grad):
    n_tok, width = tokens.shape
    hid = gate_pre.shape[1]
    rows = width // 128
    tile = width // 16
    dma = pltpu.SemaphoreType.DMA
    any_spec = pl.BlockSpec(memory_space=pl.ANY)
    vmem = pl.BlockSpec(memory_space=pltpu.VMEM)
    out = jax.ShapeDtypeStruct((rows, hid), F32)
    widths = [k[2] for k in CHUNKS]
    sums = pl.pallas_call(
        kernel,
        out_shape=(out,) * 3,
        in_specs=[any_spec] * 5,
        out_specs=(vmem,) * 3,
        scratch_shapes=[
            pltpu.VMEM((2, 8, 2 * n_tok, tile), BF16),
            pltpu.VMEM((hid // RAW, 3, 2 * n_tok, RAW), BF16),
            pltpu.VMEM((3, 2 * n_tok, hid), BF16),
            *[pltpu.VMEM((4, 4, 4, rows, w), BF16) for w in widths],
            *[pltpu.VMEM((6, 2, 4, rows, w), BF16) for w in widths],
            *[pltpu.VMEM((3, 4, rows, w) if (k, 1) in DIRECT else (6, 2, rows, w), BF16) for k, w in enumerate(widths)],
            *[pltpu.VMEM((3, rows, w) if (k, 2) in DIRECT else (6, rows // 2, w), BF16) for k, w in enumerate(widths)],
            dma((len(CHUNKS), 3)),
            dma((len(CHUNKS), 3, 2)),
            dma((3,)),
            dma((3,)),
            dma((hid // RAW + 7,)),
        ],
        compiler_params=pltpu.CompilerParams(
            collective_id=0, has_side_effects=True, vmem_limit_bytes=55850000),
        name="grad_sum",
    )(tokens, out_grad, gate_pre, up_pre, hidden_grad)
    return pl.pallas_call(
        hand_out, out_shape=(out,) * 3, in_specs=[vmem] * 3, out_specs=(any_spec,) * 3,
        scratch_shapes=[dma((3,))],
        compiler_params=pltpu.CompilerParams(vmem_limit_bytes=1 << 20), name="hand_out")(*sums)


def solution(mesh):
    split = Mesh(mesh.devices.reshape(4, 2, 4, 2, 2), AXES)
    spec_in = P(AXES, None)
    spec_out = P(("x", "yl", "c", "z", "yh"), None)
    return jax.shard_map(
        on_device, mesh=split, in_specs=(spec_in,) * 5, out_specs=(spec_out,) * 3, check_vma=False
    )
```

```python
import jax
import jax.numpy as jnp
from jax import lax
from jax.experimental import pallas as pl
from jax.experimental.pallas import tpu as pltpu
from jax.sharding import Mesh
from jax.sharding import PartitionSpec as P

AXES = ("z", "yh", "x", "yl", "c")
DIM_ORDERS = ("xyz", "yzx", "zxy", "xzy", "yxz", "zyx")
MESH = pl.DeviceIdType.MESH
F32, BF16 = jnp.float32, jnp.bfloat16

BLOCKS = (
    (0, 0, (2,), (256,)),
    (1, 0, (0,), (256,)),
    (0, 256, (1,), (256,)),
    (1, 256, (2,), (256,)),
    (0, 512, (0, 3), (128, 128)),
    (1, 512, (1,), (256,)),
    (2, 0, (2,), (256,)),
    (2, 256, (0,), (256,)),
    (2, 512, (1,), (256,)),
)
ORDER = (
    (0, 0, 0), (3, 0, 0, 0), (0, 1, 0), (3, 1, 0, 0), (0, 3, 0), (3, 3, 0, 0), (0, 2, 0), (3, 2, 0, 0),
    (0, 4, 0), (3, 5, 0, 0), (0, 4, 1), (0, 2, 1), (3, 4, 0, 1), (0, 0, 1), (3, 0, 0, 1), (3, 4, 0, 0),
    (3, 2, 0, 1), (0, 8, 0), (0, 1, 1), (0, 3, 1), (1, 5, 0), (0, 6, 0), (1, 0, 0), (3, 9, 0, 0),
    (0, 7, 0), (3, 7, 0, 0), (0, 8, 1), (3, 8, 0, 0), (1, 3, 0), (3, 9, 0, 1), (0, 0, 2), (0, 6, 1),
    (0, 7, 1), (3, 5, 0, 1), (1, 4, 0), (0, 4, 2), (0, 5, 0), (3, 1, 0, 1), (1, 2, 0), (0, 3, 2),
    (1, 8, 0), (0, 1, 2), (3, 6, 0, 0), (1, 9, 0), (3, 8, 0, 1), (2, 0, 0), (0, 5, 1), (3, 7, 0, 1),
    (0, 7, 2), (2, 5, 0), (3, 5, 1, 0), (3, 3, 0, 1), (1, 1, 0), (1, 6, 0), (2, 4, 0), (3, 0, 1, 0),
    (1, 7, 0), (3, 6, 0, 1), (0, 6, 2), (3, 4, 1, 0), (2, 3, 0), (2, 9, 0), (3, 3, 1, 0), (2, 2, 0),
    (3, 2, 1, 0), (3, 4, 1, 1), (3, 3, 1, 1), (3, 9, 1, 1), (2, 8, 0), (3, 9, 1, 0), (2, 7, 0), (3, 7, 1, 0),
    (3, 2, 1, 1), (2, 1, 0), (1, 5, 1), (3, 0, 1, 1), (3, 1, 1, 0), (3, 8, 1, 0), (2, 6, 0), (3, 6, 1, 0),
    (3, 5, 1, 1), (3, 1, 1, 1), (1, 4, 1), (1, 2, 1), (1, 0, 1), (1, 9, 1), (1, 3, 1), (1, 7, 1),
    (1, 1, 1), (3, 8, 1, 1), (3, 6, 1, 1), (3, 7, 1, 1), (2, 0, 1), (1, 8, 1), (2, 4, 1), (3, 0, 2, 0),
    (3, 4, 2, 0), (1, 6, 1), (3, 0, 2, 1), (2, 2, 1), (3, 2, 2, 0), (2, 3, 1), (2, 5, 1), (2, 9, 1),
    (3, 5, 2, 0), (3, 3, 2, 0), (3, 4, 2, 1), (3, 9, 2, 1), (3, 3, 2, 1), (3, 9, 2, 0), (2, 1, 1), (3, 1, 2, 0),
    (3, 5, 2, 1), (2, 7, 1), (3, 7, 2, 0), (3, 1, 2, 1), (1, 4, 2), (1, 2, 2), (2, 8, 1), (3, 2, 2, 1),
    (3, 8, 2, 0), (1, 0, 2), (3, 7, 2, 1), (2, 6, 1), (3, 6, 2, 0), (1, 1, 2), (3, 6, 2, 1), (3, 8, 2, 1),
    (1, 5, 2), (1, 3, 2), (2, 4, 2), (2, 0, 2), (2, 9, 2), (2, 2, 2), (2, 1, 2), (2, 5, 2),
    (2, 7, 2), (2, 3, 2), (2, 8, 2), (2, 6, 2),
)
DIRECT = ((6, 2), (7, 2), (8, 2), (9, 2))
CHUNKS = tuple(
    (b[0], b[1] + sum(b[3][:i]), w, DIM_ORDERS[b[2][i]]) for b in BLOCKS for i, w in enumerate(b[3]))
BLOCK_CHUNKS = tuple(
    tuple(sum(len(a[3]) for a in BLOCKS[:n]) + i for i in range(len(b[3]))) for n, b in enumerate(BLOCKS))
RAW = 256
PIECE = 64


def kernel(*refs):
    tokens, out_grad, gate_pre, up_pre, hidden_grad = refs[:5]
    outs = refs[5:8]
    tok, raw, hb = refs[8:11]
    n_chunk = len(CHUNKS)
    part = refs[11:11 + n_chunk]
    recv = tuple(refs[11 + (1 + ph) * n_chunk:11 + (2 + ph) * n_chunk] for ph in range(3))
    send_sem, recv_sem, in_sem, xs_sem, xr_sem = refs[11 + 4 * n_chunk:]

    z, yh, x, yl, c = (lax.axis_index(a) for a in AXES)
    y = yh * 2 + yl
    me = {"x": x, "y": y, "z": z}
    n_tok = tokens.shape[0]
    n_slot, tile = tok.shape[1], tok.shape[3]
    n_raw = raw.shape[0]
    rows = part[0].shape[3]
    step = {d: tuple(lax.rem(me[d] + k, 4) for k in range(4)) for d in "xyz"}

    def device(d, k):
        at = dict(me)
        at[d] = step[d][k]
        return (at["z"], lax.div(at["y"], 2), at["x"], lax.rem(at["y"], 2), c)

    partner = (z, yh, x, yl, 1 - c)

    def slot_at(slot):
        return lax.rem(x + 2 + lax.div(slot, 2), 4), lax.rem(yl + lax.rem(slot, 2), 2)

    barrier = pltpu.get_barrier_semaphore()
    pl.semaphore_signal(barrier, inc=1, device_id=partner, device_id_type=MESH)
    for d in "xyz":
        for k in (1, 2, 3):
            pl.semaphore_signal(barrier, inc=1, device_id=device(d, k), device_id_type=MESH)

    raws = (gate_pre, up_pre, hidden_grad)

    def pieces(core):
        found = {}
        for j in range(n_raw):
            for i, ref in enumerate(raws):
                found[("raw", j, i)] = (ref.at[:, pl.ds(j * RAW, RAW)], lambda r, j=j, i=i: raw.at[j, i, r])
        lanes = tile // 4
        for s in range(n_slot):
            sx, sl = slot_at(s)
            at = (sx * 4 + sl * 2 + core) * tile
            for k in range(4):
                src = tokens.at[:, pl.ds(pl.multiple_of(at + step["z"][k] * lanes, lanes), lanes)]
                cut = pl.ds(pl.multiple_of(step["z"][k] * lanes, lanes), lanes)
                found[("tok", s, k)] = (src, lambda r, s=s, cut=cut: tok.at[0, s, r, cut])
            src = tokens.at[:, pl.ds(pl.multiple_of(at, tile), tile)]
            found[("own", s)] = (src, lambda r, s=s: tok.at[0, s, r])
            src = out_grad.at[:, pl.ds(pl.multiple_of(at, tile), tile)]
            found[("grad", s)] = (src, lambda r, s=s: tok.at[1, s, r])
        return found

    def raw_names(j):
        return [("raw", j, i) for i in range(3)]

    def rest(slots):
        return [("tok", s, k) for s in slots for k in (0, 1, 3)]

    def grad_names(slots):
        return [("grad", s) for s in slots]

    def lanes_of(slots):
        return lambda r: tok.at[0, pl.ds(0, len(slots)), r, pl.ds(0, 3 * tile // 4)]

    def grads_of(slots):
        return lambda r: tok.at[1, pl.ds(0, len(slots)), r]

    def raw_of(j):
        return lambda r: raw.at[j, :, r]

    far_lanes = pl.ds(pl.multiple_of(step["z"][2] * (tile // 4), tile // 4), tile // 4)
    groups = [(raw_names(0), raw_of(0)),
              ([("tok", s, 2) for s in range(n_slot)], lambda r: tok.at[0, :, r, far_lanes]),
              (rest((0, 1)), lanes_of((0, 1))), (raw_names(1), raw_of(1)),
              (rest((2, 4, 6)), lanes_of((2, 4, 6))), (rest((3, 5, 7)), lanes_of((3, 5, 7)))]
    groups += [(raw_names(j), raw_of(j)) for j in range(2, n_raw)]
    groups += [(grad_names(s), grads_of(s)) for s in ((0, 1), (2, 3, 6, 7), (4, 5))]
    kinds = ("raw", "tok", "grad")
    whole = (lambda r: raw.at[:, :, r], lambda r: tok.at[0, :, r], lambda r: tok.at[1, :, r])
    first_rows, last_rows = pl.ds(0, n_tok), pl.ds(n_tok, n_tok)

    def take(ref, sem):
        pltpu.make_async_copy(ref, ref, sem).wait()

    mine, theirs = pieces(c), pieces(1 - c)
    for names, size in groups:
        for name in names:
            if name[0] != "tok":
                src, dst = mine[name]
                pltpu.make_async_copy(src, dst(first_rows), in_sem.at[kinds.index(name[0])]).start()
            elif name[2] == 2:
                src, dst = mine[("own", name[1])]
                pltpu.make_async_copy(src, dst(first_rows), in_sem.at[1]).start()

    pl.semaphore_wait(barrier, 10)

    group_of = {}
    for n, (names, size) in enumerate(groups):
        for name in names:
            group_of[name] = n
            src, dst = theirs[name]
            pltpu.make_async_remote_copy(
                src, dst(last_rows), xs_sem.at[kinds.index(name[0])], xr_sem.at[n],
                device_id=partner, device_id_type=MESH).start()

    have = set()

    def need(name):
        kind = kinds.index(name[0])
        if name[0] not in have:
            have.add(name[0])
            take(whole[kind](first_rows), in_sem.at[kind])
        n = group_of[name]
        if n not in have:
            have.add(n)
            take(groups[n][1](last_rows), xr_sem.at[n])

    def hidden(j):
        if ("hidden", j) in have:
            return
        have.add(("hidden", j))
        for i in range(3):
            need(("raw", j, i))

        def body(i, carry):
            at = pl.ds(pl.multiple_of(i * PIECE, PIECE), PIECE)
            cs = pl.ds(j * RAW, RAW)
            gate_val = raw[j, 0, at].astype(F32)
            up_val = raw[j, 1, at].astype(F32)
            grad_val = raw[j, 2, at].astype(F32)
            sig = jax.nn.sigmoid(gate_val)
            activated = gate_val * sig
            hb[2, at, cs] = (activated * up_val).astype(BF16)
            hb[1, at, cs] = (grad_val * activated).astype(BF16)
            hb[0, at, cs] = (grad_val * up_val * sig * (1.0 + gate_val * (1.0 - sig))).astype(BF16)
            return carry

        lax.fori_loop(0, 2 * n_tok // PIECE, body, 0)

    def base(k, ph):
        ref = part[k]
        for d in CHUNKS[k][3][:ph]:
            ref = ref.at[me[d]]
        return ref

    def half_of(ref, i, h):
        n = ref.shape[1] // 2
        return ref.at[i, pl.ds(h * n, n)]

    def send(k, ph, i, src, direction):
        late = 1 if i > 1 or (k, ph) in DIRECT else 0
        pltpu.make_async_remote_copy(
            src, recv[ph][k].at[i], send_sem.at[k, ph], recv_sem.at[k, ph, late],
            device_id=device(CHUNKS[k][3][ph], direction), device_id_type=MESH).start()

    def launch(k, ph, near_side):
        s = step[CHUNKS[k][3][ph]]
        b = base(k, ph)
        if (k, ph) in DIRECT:
            for i, to in ((1, 1), (2, 3)) if near_side else ((0, 2),):
                send(k, ph, i, b.at[s[to]], to)
        elif near_side:
            send(k, ph, 2, half_of(b, s[1], 1), 1)
            send(k, ph, 3, half_of(b, s[3], 0), 3)
        else:
            send(k, ph, 0, half_of(b, s[2], 0), 1)
            send(k, ph, 1, half_of(b, s[2], 1), 3)

    slots_of = (((0, 1), (2, 3, 6, 7), (4, 5)), ((0, 2, 4, 6), (1, 3, 5, 7)), (range(8),) * 3)
    pairs_of = (
        ((1, lambda i: (0, 1)), (2, lambda i: (2 + 4 * i, 3 + 4 * i)), (1, lambda i: (4, 5))),
        ((2, lambda i: (4 * i, 4 * i + 2)), (2, lambda i: (4 * i + 1, 4 * i + 3))),
    )
    z_of = ((1, lambda i: 2), (2, lambda i: 1 + 2 * i), (1, lambda i: 0))

    def multiply(b, seg):
        p, first, dim, widths = BLOCKS[b]
        dim = dim[0] % 3
        w = p // 2
        for j in range(first // RAW, (first + sum(widths) - 1) // RAW + 1):
            hidden(j)
        for s in slots_of[dim][seg]:
            if w:
                need(("grad", s))
            else:
                for k in ((2,), (1, 3), (0,))[seg] if dim == 2 else range(4):
                    need(("tok", s, k))
        count, which = (z_of if dim == 2 else pairs_of[dim])[seg]
        lanes = tile // 4

        def body(i, carry):
            if dim == 2:
                sz = lax.rem(z + which(i), 4)
                slots, levels = range(n_slot), (sz,)
                cut = pl.ds(pl.multiple_of(sz * lanes, lanes), lanes)
                left = [tok[w, s, :, cut] for s in slots]
            else:
                slots, levels = which(i), range(4)
                left = [tok[w, s] for s in slots]
            res = lax.dot_general(
                jnp.concatenate(left, axis=1), hb[p, :, pl.ds(first, sum(widths))], (((0,), (0,)), ((), ())),
                preferred_element_type=F32).astype(BF16)
            lo = 0
            for slot in slots:
                sx, sl = slot_at(slot)
                for sz in levels:
                    for sh in range(2):
                        at = {"x": sx, "y": sh * 2 + sl, "z": sz}
                        for k in BLOCK_CHUNKS[b]:
                            lane = CHUNKS[k][1] - first
                            o = CHUNKS[k][3]
                            part[k][at[o[0]], at[o[1]], at[o[2]]] = res[lo:lo + rows, lane:lane + CHUNKS[k][2]]
                        lo += rows
            return carry

        lax.fori_loop(0, count, body, 0)

    def add(first, others, dst):
        lead = dst.shape[:-2]
        count = 1
        for n in lead:
            count *= n

        def block(ix):
            v = first[ix].astype(F32)
            for o in others:
                v = v + o[ix].astype(F32)
            dst[ix] = v.astype(dst.dtype)

        if not lead:
            block((slice(None), slice(None)))
            return

        def body(i, carry):
            block((i,) if len(lead) == 1 else (lax.div(i, lead[1]), lax.rem(i, lead[1])))
            return carry

        lax.fori_loop(0, count, body, 0)

    def relay(k, ph):
        s = step[CHUNKS[k][3][ph]]
        take(recv[ph][k].at[pl.ds(0, 2)], recv_sem.at[k, ph, 0])
        for i, to in ((0, 1), (1, 3)):
            got = recv[ph][k].at[i]
            add(got, (half_of(base(k, ph), s[to], i),), got)
            send(k, ph, 4 + i, got, to)

    def finish(k, ph):
        p, first, width, o = CHUNKS[k]
        b, got, at = base(k, ph), recv[ph][k], me[o[ph]]
        cut = pl.ds(first, width)
        if (k, ph) in DIRECT:
            take(got, recv_sem.at[k, ph, 1])
            add(b.at[at], tuple(got.at[i] for i in range(3)), b.at[at] if ph < 2 else outs[p].at[:, cut])
        else:
            take(got.at[pl.ds(2, 4)], recv_sem.at[k, ph, 1])
            for h, pair in enumerate(((3, 4), (2, 5))):
                own_half = half_of(b, at, h)
                n = rows // 2
                dst = own_half if ph < 2 else outs[p].at[pl.ds(h * n, n), cut]
                add(own_half, tuple(got.at[i] for i in pair), dst)

    for op, n, m, *h in ORDER:
        (multiply, relay, finish, launch)[op](n, m, *h)

    for kind in range(3):
        take(whole[kind](first_rows), xs_sem.at[kind])
    for k in range(n_chunk):
        ref = part[k]
        for ph in range(3):
            take(ref.at[pl.ds(0, 3)], send_sem.at[k, ph])
            ref = ref.at[0]


def hand_out(*refs):
    copies = [pltpu.make_async_copy(refs[p], refs[3 + p], refs[6].at[p]) for p in range(3)]
    for cp in copies:
        cp.start()
    for cp in copies:
        cp.wait()


def on_device(tokens, out_grad, gate_pre, up_pre, hidden_grad):
    n_tok, width = tokens.shape
    hid = gate_pre.shape[1]
    rows = width // 128
    tile = width // 16
    dma = pltpu.SemaphoreType.DMA
    any_spec = pl.BlockSpec(memory_space=pl.ANY)
    vmem = pl.BlockSpec(memory_space=pltpu.VMEM)
    out = jax.ShapeDtypeStruct((rows, hid), F32)
    widths = [k[2] for k in CHUNKS]
    sums = pl.pallas_call(
        kernel,
        out_shape=(out,) * 3,
        in_specs=[any_spec] * 5,
        out_specs=(vmem,) * 3,
        scratch_shapes=[
            pltpu.VMEM((2, 8, 2 * n_tok, tile), BF16),
            pltpu.VMEM((hid // RAW, 3, 2 * n_tok, RAW), BF16),
            pltpu.VMEM((3, 2 * n_tok, hid), BF16),
            *[pltpu.VMEM((4, 4, 4, rows, w), BF16) for w in widths],
            *[pltpu.VMEM((6, 2, 4, rows, w), BF16) for w in widths],
            *[pltpu.VMEM((3, 4, rows, w) if (k, 1) in DIRECT else (6, 2, rows, w), BF16) for k, w in enumerate(widths)],
            *[pltpu.VMEM((3, rows, w) if (k, 2) in DIRECT else (6, rows // 2, w), BF16) for k, w in enumerate(widths)],
            dma((len(CHUNKS), 3)),
            dma((len(CHUNKS), 3, 2)),
            dma((3,)),
            dma((3,)),
            dma((hid // RAW + 7,)),
        ],
        compiler_params=pltpu.CompilerParams(
            collective_id=0, has_side_effects=True, vmem_limit_bytes=55850000),
        name="grad_sum",
    )(tokens, out_grad, gate_pre, up_pre, hidden_grad)
    return pl.pallas_call(
        hand_out, out_shape=(out,) * 3, in_specs=[vmem] * 3, out_specs=(any_spec,) * 3,
        scratch_shapes=[dma((3,))],
        compiler_params=pltpu.CompilerParams(vmem_limit_bytes=1 << 20), name="hand_out")(*sums)


def solution(mesh):
    split = Mesh(mesh.devices.reshape(4, 2, 4, 2, 2), AXES)
    spec_in = P(AXES, None)
    spec_out = P(("x", "yl", "c", "z", "yh"), None)
    return jax.shard_map(
        on_device, mesh=split, in_specs=(spec_in,) * 5, out_specs=(spec_out,) * 3, check_vma=False
    )
```
